32 devices in a mesh: dp: 16 (over z, y, x), tensor: 2 (over core).
Axes of the slice: x: 2, y: 2, z: 4, core: 2. Of those that a mesh axis runs over, the one named last changes fastest.
Arguments:
- layer_input: bfloat16 [16384, 768], P('dp'), may hold values from -6 to 6
- patch_features: bfloat16 [16384, 1024], P('dp', 'tensor'), may hold values from -400 to 400
- bucket_ids: int32 [64], P('dp'), may hold values from 0 to 1
- text_lengths: int32 [64], P('dp'), may hold values from 1 to 31
- upstream: bfloat16 [16384, 768], P('dp'), may hold values from -6 to 6
- query_weight: bfloat16 [768, 768], P(None, 'tensor'), may hold values from -0.21875 to 0.21875
- key_weight: bfloat16 [768, 768], P(None, 'tensor'), may hold values from -0.21875 to 0.21875
- value_weight: bfloat16 [768, 768], P(None, 'tensor'), may hold values from -0.21875 to 0.21875
- merge_weight: bfloat16 [768, 768], P('tensor'), may hold values from -1.75 to 1.75
- query_bias: float32 [768], P('tensor'), may hold values from -3 to 3
- value_bias: float32 [768], P('tensor'), may hold values from -3 to 3
- merge_bias: float32 [768], replicated, may hold values from -3 to 3
- head_gain: float32 [12], P('tensor'), may hold values from 0.25 to 1.75
- distance_table: float32 [12, 511], P('tensor'), may hold values from -4 to 4
- first_gain: float32 [768], replicated, may hold values from 0.25 to 1.75
- first_shift: float32 [768], replicated, may hold values from -3 to 3
- second_gain: float32 [768], replicated, may hold values from 0.25 to 1.75
- second_shift: float32 [768], replicated, may hold values from -3 to 3
- expand_weight: bfloat16 [768, 3072], P(None, 'tensor'), may hold values from -0.21875 to 0.21875
- expand_bias: float32 [3072], P('tensor'), may hold values from -3 to 3
- reduce_weight: bfloat16 [3072, 768], P('tensor'), may hold values from -0.15625 to 0.15625
- reduce_bias: float32 [768], replicated, may hold values from -3 to 3
- image_weight: bfloat16 [1024, 768], P('tensor'), may hold values from -0.1875 to 0.1875
- stem_gain: float32 [1024], P('tensor'), may hold values from 0.25 to 1.75
- stem_shift: float32 [1024], P('tensor'), may hold values from -3 to 3
Outputs:
- block_output: bfloat16 [16384, 768], P('dp')
- input_grad: float32 [16384, 768], P('dp')
- patch_grad: float32 [16384, 1024], P('dp', 'tensor')
- grad_query_weight: float32 [768, 768], P(None, 'tensor')
- grad_key_weight: float32 [768, 768], P(None, 'tensor')
- grad_value_weight: float32 [768, 768], P(None, 'tensor')
- grad_merge_weight: float32 [768, 768], P('tensor')
- grad_query_bias: float32 [768], P('tensor')
- grad_value_bias: float32 [768], P('tensor')
- grad_merge_bias: float32 [768], replicated
- grad_head_gain: float32 [12], P('tensor')
- grad_distance_table: float32 [12, 511], P('tensor')
- grad_first_gain: float32 [768], replicated
- grad_first_shift: float32 [768], replicated
- grad_second_gain: float32 [768], replicated
- grad_second_shift: float32 [768], replicated
- grad_expand_weight: float32 [768, 3072], P(None, 'tensor')
- grad_expand_bias: float32 [3072], P('tensor')
- grad_reduce_weight: float32 [3072, 768], P('tensor')
- grad_reduce_bias: float32 [768], replicated
- grad_image_weight: float32 [1024, 768], P('tensor')
- grad_stem_gain: float32 [1024], P('tensor')
- grad_stem_shift: float32 [1024], P('tensor')
The draws below stay inside these ranges and needn't reach their ends.
All inputs are finite; a program needn't handle non-finite values.
Results may differ from the reference program's by a relative error of at most 0.014.
Values sent between devices are 32-bit elements; how exact they have to be, the bound alone decides.
No kernel may reach another device: no remote copies, remote signals or barrier semaphores. Data moves between devices by JAX's collectives and lax.ppermute only.
A program may use at most 128 MiB of HBM per device.

```python
import math
import jax
import jax.numpy as jnp
from jax import lax

D = 768
HEADS = 12
HEAD_DIM = 64
FF = 3072
CH = 1024
SEQ = 256
PATCH_SMALL = 64
PATCH_LARGE = 225
TEXT_MAX = 31
NREL = 511
ITEMS = 64
TOKENS = 16384


def draw_patch_features(key, part):
    subkeys = jax.random.split(key, 3)
    channel_scale = jnp.exp(jax.random.uniform(subkeys[0], (CH,), jnp.float32, 0.0, math.log(10.0)))
    channel_mean = 2.0 * jnp.clip(jax.random.normal(subkeys[1], (CH,), jnp.float32), -2.0, 2.0)
    item_index = (jnp.arange(TOKENS) // SEQ).astype(jnp.float32)
    ramp = 1.0 + 2.0 * item_index / max(ITEMS - 1, 1)
    noise = jnp.clip(jax.random.normal(subkeys[2], (TOKENS, CH), jnp.float32), -4.0, 4.0)
    return ((channel_mean[None, :] + noise * ramp[:, None]) * channel_scale[None, :]).astype(jnp.bfloat16)


def draw_bucket_ids(key, part):
    drawn = jax.random.randint(jax.random.fold_in(key, 11), (ITEMS,), 0, 2, dtype=jnp.int32)
    return drawn.at[0].set(1).at[ITEMS - 1].set(0)


def draw_text_lengths(key, part):
    drawn = jax.random.randint(jax.random.fold_in(key, 23), (ITEMS,), 1, TEXT_MAX + 1, dtype=jnp.int32)
    return drawn.at[0].set(TEXT_MAX).at[ITEMS - 1].set(1)


def block_scale(stream_key, dims, shards, smallest, largest):
    factor_of, own = 1.0, jax.random.fold_in(stream_key, 6)
    for dim, parts in shards:
        heights = jnp.exp(jax.random.uniform(jax.random.fold_in(own, dim), (parts,), jnp.float32, smallest / len(shards), largest / len(shards)))
        factor_of = factor_of * jnp.repeat(heights, dims[dim] // parts).reshape([-1 if axis == dim else 1 for axis in range(len(dims))])
    return factor_of


def gaussian(stream_key, shape, spread, most, shards=(), held_as=jnp.bfloat16):
    factor_of = block_scale(stream_key, shape, shards, -0.22, 0.18) if shards else 1.0
    values = jax.random.normal(stream_key, shape, jnp.float32) * spread * factor_of
    return jnp.minimum(jnp.maximum(values, -most), most).astype(held_as)


def setup_inputs(seed: int = 0) -> dict:
    seeds = jax.random.split(jax.random.key(seed), 26)
    layer_input = gaussian(seeds[0], (TOKENS, D), 1.0, 6.0, ((0, 16),))
    patch_features = draw_patch_features(jax.random.fold_in(seeds[25], 71), 0)
    bucket_ids = draw_bucket_ids(jax.random.fold_in(seeds[25], 71), 0)
    text_lengths = draw_text_lengths(jax.random.fold_in(seeds[25], 71), 0)
    upstream = gaussian(seeds[4], (TOKENS, D), 1.0, 6.0, ((0, 16),))
    query_weight = gaussian(seeds[5], (D, D), D ** -0.5, 0.21875, ((1, 2),))
    key_weight = gaussian(seeds[6], (D, D), D ** -0.5, 0.21875, ((1, 2),))
    value_weight = gaussian(seeds[7], (D, D), D ** -0.5, 0.21875, ((1, 2),))
    merge_weight = gaussian(seeds[8], (D, D), (4 * D // SEQ) ** -0.5, 1.75, ((0, 2),))
    query_bias = gaussian(seeds[9], (D,), 0.5, 3.0, ((0, 2),), jnp.float32)
    value_bias = gaussian(seeds[10], (D,), 0.5, 3.0, ((0, 2),), jnp.float32)
    merge_bias = gaussian(seeds[11], (D,), 0.5, 3.0, (), jnp.float32)
    head_gain = jnp.clip(1.0 + 0.15 * jax.random.normal(seeds[12], (HEADS,), jnp.float32), 0.25, 1.75)
    distance_table = gaussian(seeds[13], (HEADS, NREL), 1.0, 4.0, ((0, 2),), jnp.float32)
    first_gain = jnp.clip(1.0 + 0.15 * jax.random.normal(seeds[14], (D,), jnp.float32), 0.25, 1.75)
    first_shift = gaussian(seeds[15], (D,), 0.5, 3.0, (), jnp.float32)
    second_gain = jnp.clip(1.0 + 0.15 * jax.random.normal(seeds[16], (D,), jnp.float32), 0.25, 1.75)
    second_shift = gaussian(seeds[17], (D,), 0.5, 3.0, (), jnp.float32)
    expand_weight = gaussian(seeds[18], (D, FF), D ** -0.5, 0.21875, ((1, 2),))
    expand_bias = gaussian(seeds[19], (FF,), 0.5, 3.0, ((0, 2),), jnp.float32)
    reduce_weight = gaussian(seeds[20], (FF, D), (FF // 2) ** -0.5, 0.15625, ((0, 2),))
    reduce_bias = gaussian(seeds[21], (D,), 0.5, 3.0, (), jnp.float32)
    image_weight = gaussian(seeds[22], (CH, D), CH ** -0.5, 0.1875, ((0, 2),))
    stem_gain = jnp.clip(1.0 + 0.15 * jax.random.normal(seeds[23], (CH,), jnp.float32), 0.25, 1.75)
    stem_shift = gaussian(seeds[24], (CH,), 0.5, 3.0, ((0, 2),), jnp.float32)
    return dict(layer_input=layer_input, patch_features=patch_features, bucket_ids=bucket_ids, text_lengths=text_lengths, upstream=upstream, query_weight=query_weight, key_weight=key_weight, value_weight=value_weight, merge_weight=merge_weight, query_bias=query_bias, value_bias=value_bias, merge_bias=merge_bias, head_gain=head_gain, distance_table=distance_table, first_gain=first_gain, first_shift=first_shift, second_gain=second_gain, second_shift=second_shift, expand_weight=expand_weight, expand_bias=expand_bias, reduce_weight=reduce_weight, reduce_bias=reduce_bias, image_weight=image_weight, stem_gain=stem_gain, stem_shift=stem_shift)


@jax.custom_vjp
def low(v):
    return lax.optimization_barrier(v.astype(jnp.bfloat16)).astype(jnp.float32)

@jax.custom_vjp
def low_back(v):
    return v

def low_keep(v):
    return (low(v), None)

def low_pass(kept, grad):
    return (grad,)

def back_keep(v):
    return (v, None)

def back_low(kept, grad):
    return (low(grad),)
low.defvjp(low_keep, low_pass)
low_back.defvjp(back_keep, back_low)
EPSILON = 1e-05
NEGATIVE = -1e+30

def highest(left, right):
    return jnp.dot(left, right, precision=lax.Precision.HIGHEST, preferred_element_type=jnp.float32)

def layer_norm(values, gain, shift):
    centered = values - lax.optimization_barrier(jnp.mean(values, axis=-1, keepdims=True))
    scaled = centered * lax.rsqrt(lax.optimization_barrier(jnp.mean(centered * centered, axis=-1, keepdims=True)) + EPSILON)
    return scaled * gain + shift

def block(layer_input, patch_features, query_weight, key_weight, value_weight, merge_weight, query_bias, value_bias, merge_bias, head_gain, distance_table, first_gain, first_shift, second_gain, second_shift, expand_weight, expand_bias, reduce_weight, reduce_bias, image_weight, stem_gain, stem_shift, patch_mask, valid):
    count = jnp.sum(patch_mask)
    column = patch_mask[:, None]
    masked = patch_features * column
    stem_mean = lax.optimization_barrier(jnp.sum(masked, axis=0)) / count
    stem_square = lax.optimization_barrier(jnp.sum(masked * patch_features, axis=0)) / count
    stem_inverse = lax.rsqrt(stem_square - stem_mean * stem_mean + EPSILON)
    normed = (patch_features - stem_mean) * stem_inverse * stem_gain + stem_shift
    embedded = low_back(highest(low(normed), image_weight))
    hidden = layer_input + column * embedded
    first = low(layer_norm(hidden, first_gain, first_shift))
    queries = low(low_back(highest(first, query_weight) + query_bias))
    keyed = low(low_back(highest(first, key_weight)))
    values = low(low_back(highest(first, value_weight) + value_bias))
    split_shape = (ITEMS, SEQ, HEADS, HEAD_DIM)
    offsets = jnp.arange(SEQ, dtype=jnp.int32)[None, :] - jnp.arange(SEQ, dtype=jnp.int32)[:, None] + SEQ - 1
    bias = distance_table[:, offsets]
    scale = HEAD_DIM ** (-0.5)

    def attend(pieces):
        item_queries, item_keys, item_values, item_valid = pieces
        scores = jnp.einsum('qhd,khd->hqk', item_queries, item_keys, precision=lax.Precision.HIGHEST) * scale + bias
        scores = low_back(jnp.where(item_valid[None, None, :], scores, NEGATIVE))
        probs = jax.nn.softmax(scores, axis=-1)
        return jnp.einsum('hqk,khd->qhd', low(probs), item_values, precision=lax.Precision.HIGHEST)
    mixed = lax.map(jax.checkpoint(attend), (queries.reshape(split_shape), keyed.reshape(split_shape), values.reshape(split_shape), valid))
    mixed = low_back(mixed)
    scaled = low(mixed * head_gain[None, None, :, None]).reshape(TOKENS, D)
    middle = hidden + low_back(highest(scaled, merge_weight)) + merge_bias
    second = low(layer_norm(middle, second_gain, second_shift))
    expanded = low_back(highest(second, expand_weight) + expand_bias)
    active = low(jax.nn.gelu(expanded, approximate=False))
    return middle + low_back(highest(active, reduce_weight)) + reduce_bias

def reference(layer_input, patch_features, bucket_ids, text_lengths, upstream, query_weight, key_weight, value_weight, merge_weight, query_bias, value_bias, merge_bias, head_gain, distance_table, first_gain, first_shift, second_gain, second_shift, expand_weight, expand_bias, reduce_weight, reduce_bias, image_weight, stem_gain, stem_shift):
    patches = PATCH_SMALL + (PATCH_LARGE - PATCH_SMALL) * bucket_ids
    slots = jnp.arange(SEQ, dtype=jnp.int32)
    patch_mask = (slots[None, :] < patches[:, None]).astype(jnp.float32).reshape(TOKENS)
    valid = slots[None, :] < (patches + text_lengths)[:, None]
    valid_rows = valid.astype(jnp.float32).reshape(TOKENS)
    floats = (layer_input, patch_features, query_weight, key_weight, value_weight, merge_weight, query_bias, value_bias, merge_bias, head_gain, distance_table, first_gain, first_shift, second_gain, second_shift, expand_weight, expand_bias, reduce_weight, reduce_bias, image_weight, stem_gain, stem_shift)
    floats = tuple((entry.astype(jnp.float32) for entry in floats))

    def forward(*params):
        return block(*params, patch_mask, valid)
    result, pullback = jax.vjp(forward, *floats)
    grads = pullback(upstream.astype(jnp.float32) * valid_rows[:, None])
    return (result.astype(jnp.bfloat16), grads[0], grads[1], grads[2], grads[3], grads[4], grads[5], grads[6], grads[7], grads[8], grads[9], grads[10], grads[11], grads[12], grads[13], grads[14], grads[15], grads[16], grads[17], grads[18], grads[19], grads[20], grads[21])
```

```python
from functools import partial

import jax
import jax.numpy as jnp
from jax import lax
from jax.sharding import PartitionSpec as P

HEAD_DIM = 64
PATCH_SMALL = 64
PATCH_LARGE = 225


EPSILON = 1e-05
NEGATIVE = -1e30


def layer_norm(values, gain, shift):
    centered = values - jnp.mean(values, axis=-1, keepdims=True)
    scaled = centered * lax.rsqrt(jnp.mean(centered * centered, axis=-1, keepdims=True) + EPSILON)
    return scaled * gain + shift


def distance_bias(table, length):
    count_heads = table.shape[0]
    padded = jnp.pad(table, ((0, 0), (0, 1)))
    tiled = jnp.broadcast_to(padded[:, None, :], (count_heads, length, 2 * length)).reshape(
        count_heads, 2 * length * length
    )
    window = tiled[:, length - 1 : length - 1 + length * (2 * length - 1)].reshape(
        count_heads, length, 2 * length - 1
    )
    return window[:, :, :length]


def scores_of(query_low, key_low, bias, key_valid, scale):
    scores = (
        jnp.einsum("bqhd,bkhd->bhqk", query_low, key_low, preferred_element_type=jnp.float32)
        * scale
        + bias[None]
    )
    return jnp.where(key_valid[:, None, None, :], scores, NEGATIVE)


def project_back(grad_low, weight):
    return jnp.einsum("tf,df->td", grad_low, weight, preferred_element_type=jnp.float32)


def weight_grad(inputs_low, grad_low):
    return jnp.einsum("tc,td->cd", inputs_low, grad_low, preferred_element_type=jnp.float32)


def swap_core(values):
    count = lax.axis_size("tensor")
    pairs = [(core, core ^ 1) for core in range(count)]
    return values + lax.ppermute(values, "tensor", pairs)


def exchange(values, bit):
    count = lax.axis_size("dp")
    pairs = [(rank, rank ^ (1 << bit)) for rank in range(count)]
    return lax.ppermute(values, "dp", pairs)


def sum_by_doubling(values):
    for bit in range(lax.axis_size("dp").bit_length() - 1):
        values = values + exchange(values, bit)
    return values


def sum_by_halving(values, order):
    rank = lax.axis_index("dp")
    for bit in order:
        half = values.shape[0] // 2
        side = (rank >> bit) & 1
        sent = lax.dynamic_slice_in_dim(values, (1 - side) * half, half, 0)
        kept = lax.dynamic_slice_in_dim(values, side * half, half, 0)
        values = kept + exchange(sent, bit)
    for bit in reversed(order):
        side = (rank >> bit) & 1
        other = exchange(values, bit)
        values = jnp.where(
            side == 1, jnp.concatenate([other, values]), jnp.concatenate([values, other])
        )
    return values


def orders():
    bits = tuple(range(lax.axis_size("dp").bit_length() - 1))
    return bits, (bits[1], bits[0]) + bits[2:]


def pack(arrays):
    flat = jnp.concatenate([entry.reshape(-1) for entry in arrays])
    short = -flat.shape[0] % 1024
    return jnp.pad(flat, (0, short)).reshape(-1, 128)


def unpack(packed, arrays):
    flat, at, parts = packed.reshape(-1), 0, []
    for entry in arrays:
        parts.append(flat[at : at + entry.size].reshape(entry.shape))
        at += entry.size
    return parts


def local(
    layer_input,
    patch_features,
    bucket_ids,
    text_lengths,
    upstream,
    query_weight,
    key_weight,
    value_weight,
    merge_weight,
    query_bias,
    value_bias,
    merge_bias,
    head_gain,
    distance_table,
    first_gain,
    first_shift,
    second_gain,
    second_shift,
    expand_weight,
    expand_bias,
    reduce_weight,
    reduce_bias,
    image_weight,
    stem_gain,
    stem_shift,
):
    items = bucket_ids.shape[0]
    rows = layer_input.shape[0]
    length = rows // items
    heads = head_gain.shape[0]
    width = query_weight.shape[1]
    scale = HEAD_DIM ** (-0.5)
    patches = PATCH_SMALL + (PATCH_LARGE - PATCH_SMALL) * bucket_ids
    slots = jnp.arange(length, dtype=jnp.int32)
    patch_mask = (slots[None, :] < patches[:, None]).astype(jnp.float32).reshape(rows)
    key_valid = slots[None, :] < (patches + text_lengths)[:, None]
    valid_rows = key_valid.astype(jnp.float32).reshape(rows)
    features = patch_features.astype(jnp.float32)
    masked = features * patch_mask[:, None]
    feature_sum, square_sum, count = sum_by_doubling(
        jnp.stack(
            [
                jnp.sum(masked, axis=0),
                jnp.sum(masked * features, axis=0),
                jnp.full((features.shape[1],), jnp.sum(patch_mask)),
            ]
        )
    )
    stem_mean = feature_sum / count
    stem_inverse = lax.rsqrt(square_sum / count - stem_mean * stem_mean + EPSILON)
    stem_hat = (features - stem_mean) * stem_inverse
    stem_low = (stem_hat * stem_gain + stem_shift).astype(jnp.bfloat16)
    embedded = swap_core(jnp.dot(stem_low, image_weight, preferred_element_type=jnp.float32))
    hidden = layer_input.astype(jnp.float32) + patch_mask[:, None] * embedded
    first_normed, first_back = jax.vjp(layer_norm, hidden, first_gain, first_shift)
    first_low = first_normed.astype(jnp.bfloat16)
    split_shape = (items, length, heads, HEAD_DIM)
    query_low = (
        (jnp.dot(first_low, query_weight, preferred_element_type=jnp.float32) + query_bias)
        .astype(jnp.bfloat16)
        .reshape(split_shape)
    )
    key_low = (
        jnp.dot(first_low, key_weight, preferred_element_type=jnp.float32)
        .astype(jnp.bfloat16)
        .reshape(split_shape)
    )
    value_low = (
        (jnp.dot(first_low, value_weight, preferred_element_type=jnp.float32) + value_bias)
        .astype(jnp.bfloat16)
        .reshape(split_shape)
    )
    bias, bias_back = jax.vjp(lambda table: distance_bias(table, length), distance_table)
    scores = scores_of(query_low, key_low, bias, key_valid, scale)
    peak = jnp.max(scores, axis=-1, keepdims=True)
    log_total = peak + jnp.log(jnp.sum(jnp.exp(scores - peak), axis=-1, keepdims=True))
    probs_low = jnp.exp(scores - log_total).astype(jnp.bfloat16)
    mixed = jnp.einsum("bhqk,bkhd->bqhd", probs_low, value_low, preferred_element_type=jnp.float32)
    scaled_low = (mixed * head_gain[None, None, :, None]).astype(jnp.bfloat16).reshape(rows, width)
    branch = swap_core(jnp.dot(scaled_low, merge_weight, preferred_element_type=jnp.float32))
    middle = hidden + branch + merge_bias
    second_normed, second_back = jax.vjp(layer_norm, middle, second_gain, second_shift)
    second_low = second_normed.astype(jnp.bfloat16)
    expanded = jnp.dot(second_low, expand_weight, preferred_element_type=jnp.float32) + expand_bias
    active, gelu_back = jax.vjp(partial(jax.nn.gelu, approximate=False), expanded)
    active_low = active.astype(jnp.bfloat16)
    reduced = swap_core(jnp.dot(active_low, reduce_weight, preferred_element_type=jnp.float32))
    block_output = (middle + reduced + reduce_bias).astype(jnp.bfloat16)
    grad_result = upstream.astype(jnp.float32) * valid_rows[:, None]
    grad_reduce_bias = jnp.sum(grad_result, axis=0)
    grad_reduced_low = grad_result.astype(jnp.bfloat16)
    grad_reduce_weight = weight_grad(active_low, grad_reduced_low)
    (grad_expanded,) = gelu_back(project_back(grad_reduced_low, reduce_weight))
    grad_expanded_low = grad_expanded.astype(jnp.bfloat16)
    grad_expand_bias = jnp.sum(grad_expanded_low.astype(jnp.float32), axis=0)
    grad_expand_weight = weight_grad(second_low, grad_expanded_low)
    grad_second = swap_core(project_back(grad_expanded_low, expand_weight))
    grad_middle_part, grad_second_gain, grad_second_shift = second_back(grad_second)
    grad_middle = grad_result + grad_middle_part
    grad_merge_bias = jnp.sum(grad_middle, axis=0)
    grad_branch_low = grad_middle.astype(jnp.bfloat16)
    grad_merge_weight = weight_grad(scaled_low, grad_branch_low)
    grad_scaled = project_back(grad_branch_low, merge_weight).reshape(split_shape)
    grad_head_gain = jnp.sum(grad_scaled * mixed, axis=(0, 1, 3))
    grad_mixed_low = (grad_scaled * head_gain[None, None, :, None]).astype(jnp.bfloat16)
    again = scores_of(query_low, key_low, bias, key_valid, scale)
    probs = jnp.exp(again - log_total)
    probs_again = probs.astype(jnp.bfloat16)
    grad_value_low = jnp.einsum(
        "bhqk,bqhd->bkhd", probs_again, grad_mixed_low, preferred_element_type=jnp.float32
    ).astype(jnp.bfloat16)
    grad_probs = jnp.einsum(
        "bqhd,bkhd->bhqk", grad_mixed_low, value_low, preferred_element_type=jnp.float32
    )
    grad_scores = probs * (grad_probs - jnp.sum(probs * grad_probs, axis=-1, keepdims=True))
    grad_scores_low = grad_scores.astype(jnp.bfloat16)
    (grad_distance_table,) = bias_back(jnp.sum(grad_scores_low.astype(jnp.float32), axis=0))
    grad_query_low = (
        (
            jnp.einsum(
                "bhqk,bkhd->bqhd", grad_scores_low, key_low, preferred_element_type=jnp.float32
            )
            * scale
        )
        .astype(jnp.bfloat16)
        .reshape(rows, width)
    )
    grad_key_low = (
        (
            jnp.einsum(
                "bhqk,bqhd->bkhd", grad_scores_low, query_low, preferred_element_type=jnp.float32
            )
            * scale
        )
        .astype(jnp.bfloat16)
        .reshape(rows, width)
    )
    grad_value_low = grad_value_low.reshape(rows, width)
    grad_query_bias = jnp.sum(grad_query_low.astype(jnp.float32), axis=0)
    grad_value_bias = jnp.sum(grad_value_low.astype(jnp.float32), axis=0)
    grad_heads_low = jnp.concatenate([grad_query_low, grad_key_low, grad_value_low], axis=1)
    grad_heads_weight = weight_grad(first_low, grad_heads_low)
    grad_first_part = (
        project_back(grad_query_low, query_weight)
        + project_back(grad_key_low, key_weight)
        + project_back(grad_value_low, value_weight)
    )
    grad_first = swap_core(grad_first_part)
    grad_hidden_part, grad_first_gain, grad_first_shift = first_back(grad_first)
    input_grad = grad_middle + grad_hidden_part
    grad_embedded_low = (input_grad * patch_mask[:, None]).astype(jnp.bfloat16)
    grad_image_weight = weight_grad(stem_low, grad_embedded_low)
    grad_stem = project_back(grad_embedded_low, image_weight)
    shift_local = jnp.sum(grad_stem, axis=0)
    gain_local = jnp.sum(grad_stem * stem_hat, axis=0)
    first_order, second_order = orders()
    grad_reduce_weight = lax.psum(grad_reduce_weight, "dp")
    grad_expand_weight = sum_by_halving(grad_expand_weight, second_order)
    merge_rows = grad_merge_weight.shape[0]
    row_weights = sum_by_halving(
        jnp.concatenate([grad_merge_weight, grad_image_weight]), second_order
    )
    grad_merge_weight, grad_image_weight = row_weights[:merge_rows], row_weights[merge_rows:]
    grad_heads_weight = sum_by_halving(grad_heads_weight, first_order)
    grad_query_weight = grad_heads_weight[:, :width]
    grad_key_weight = grad_heads_weight[:, width : 2 * width]
    grad_value_weight = grad_heads_weight[:, 2 * width :]
    small = (
        grad_query_bias,
        grad_value_bias,
        grad_merge_bias,
        grad_head_gain,
        grad_distance_table,
        grad_first_gain,
        grad_first_shift,
        grad_second_gain,
        grad_second_shift,
        grad_expand_bias,
        grad_reduce_bias,
        gain_local,
        shift_local,
    )
    (
        grad_query_bias,
        grad_value_bias,
        grad_merge_bias,
        grad_head_gain,
        grad_distance_table,
        grad_first_gain,
        grad_first_shift,
        grad_second_gain,
        grad_second_shift,
        grad_expand_bias,
        grad_reduce_bias,
        grad_stem_gain,
        grad_stem_shift,
    ) = unpack(sum_by_doubling(pack(small)), small)
    patch_grad = (
        patch_mask[:, None]
        * stem_inverse
        * stem_gain
        * (grad_stem - grad_stem_shift / count - stem_hat * grad_stem_gain / count)
    )
    return (
        block_output,
        input_grad,
        patch_grad,
        grad_query_weight,
        grad_key_weight,
        grad_value_weight,
        grad_merge_weight,
        grad_query_bias,
        grad_value_bias,
        grad_merge_bias,
        grad_head_gain,
        grad_distance_table,
        grad_first_gain,
        grad_first_shift,
        grad_second_gain,
        grad_second_shift,
        grad_expand_weight,
        grad_expand_bias,
        grad_reduce_weight,
        grad_reduce_bias,
        grad_image_weight,
        grad_stem_gain,
        grad_stem_shift,
    )


def solution(mesh):
    in_specs = (
        P("dp", None),
        P("dp", "tensor"),
        P("dp"),
        P("dp"),
        P("dp", None),
        P(None, "tensor"),
        P(None, "tensor"),
        P(None, "tensor"),
        P("tensor", None),
        P("tensor"),
        P("tensor"),
        P(),
        P("tensor"),
        P("tensor", None),
        P(),
        P(),
        P(),
        P(),
        P(None, "tensor"),
        P("tensor"),
        P("tensor", None),
        P(),
        P("tensor", None),
        P("tensor"),
        P("tensor"),
    )
    out_specs = (
        P("dp", None),
        P("dp", None),
        P("dp", "tensor"),
        P(None, "tensor"),
        P(None, "tensor"),
        P(None, "tensor"),
        P("tensor", None),
        P("tensor"),
        P("tensor"),
        P(),
        P("tensor"),
        P("tensor", None),
        P(),
        P(),
        P(),
        P(),
        P(None, "tensor"),
        P("tensor"),
        P("tensor", None),
        P(),
        P("tensor", None),
        P("tensor"),
        P("tensor"),
    )
    return jax.shard_map(local, mesh=mesh, in_specs=in_specs, out_specs=out_specs, check_vma=False)
```

```python
from functools import partial

import jax
import jax.numpy as jnp
from jax import lax
from jax.experimental import pallas as pl
from jax.experimental.pallas import tpu as pltpu
from jax.sharding import PartitionSpec as P

HEAD_DIM = 64
PATCH_SMALL = 64
PATCH_LARGE = 225
EPSILON = 1e-05
NEGATIVE = -1e30
SCALE = HEAD_DIM ** (-0.5)
LANES = 128
FULL = ((1,), (0,))
RIGHT = ((1,), (1,))
LEFT = ((0,), (0,))


def mult(left, right, dims=FULL):
    return lax.dot_general(left, right, (dims, ((), ())), preferred_element_type=jnp.float32)


def rows_of(length):
    return pl.BlockSpec((length[0], length[1]), lambda item, *_: (item, 0))


def whole(shape):
    return pl.BlockSpec(shape, lambda item, *_: (0,) * len(shape))


def normed(values):
    centered = values - jnp.mean(values, axis=-1, keepdims=True)
    inverse = lax.rsqrt(jnp.mean(centered * centered, axis=-1, keepdims=True) + EPSILON)
    return centered * inverse, inverse


def before(length, limit):
    slots = lax.broadcasted_iota(jnp.int32, (length, 1), 0)
    return jnp.where(slots < limit, 1.0, 0.0).astype(jnp.float32)


def norm_back(normal, inverse, grad, gain):
    scaled = grad * gain
    first = jnp.mean(scaled, axis=-1, keepdims=True)
    second = jnp.mean(scaled * normal, axis=-1, keepdims=True)
    return (scaled - first - normal * second) * inverse


def row_sum(values):
    return jnp.sum(values, axis=0, keepdims=True)


def start_sums(*refs):
    @pl.when(pl.program_id(0) == 0)
    def _():
        for ref in refs:
            ref[...] = jnp.zeros(ref.shape, ref.dtype)


def bias_kernel(table_ref, out_ref):
    length = out_ref.shape[1]
    for head in range(out_ref.shape[0]):
        rows = jnp.broadcast_to(table_ref[head : head + 1, :], (length, 2 * length))
        turned = pltpu.roll(rows, length + 1, 1, stride=1, stride_axis=0)
        out_ref[head] = turned[:, :length]


def distance_bias(table, length):
    heads = table.shape[0]
    padded = jnp.pad(table, ((0, 0), (0, 2 * length - table.shape[1])))
    return pl.pallas_call(
        bias_kernel,
        out_shape=jax.ShapeDtypeStruct((heads, length, length), jnp.float32),
        name="distance_bias",
    )(padded)


def half_of(pair, side):
    lanes = lax.broadcasted_iota(jnp.int32, pair.shape, 1)
    keep = lanes < HEAD_DIM if side == 0 else lanes >= HEAD_DIM
    return jnp.where(keep, pair, jnp.zeros_like(pair))


def join(left, right):
    lanes = lax.broadcasted_iota(jnp.int32, left.shape, 1)
    return jnp.where(lanes < HEAD_DIM, left, right)


def attend_kernel(
    patches_ref,
    valid_ref,
    input_ref,
    own_ref,
    other_ref,
    gain_ref,
    shift_ref,
    heads_weight_ref,
    heads_bias_ref,
    bias_ref,
    head_gain_ref,
    merge_ref,
    hidden_ref,
    first_ref,
    heads_ref,
    probs_ref,
    mixed_ref,
    scaled_ref,
    branch_ref,
):
    item = pl.program_id(0)
    length = input_ref.shape[0]
    width = mixed_ref.shape[1]
    mask = before(length, patches_ref[item])
    hidden = input_ref[...].astype(jnp.float32) + mask * (own_ref[...] + other_ref[...])
    hidden_ref[...] = hidden
    normal, _ = normed(hidden)
    first = (normal * gain_ref[...] + shift_ref[...]).astype(jnp.bfloat16)
    first_ref[...] = first
    heads_ref[...] = (mult(first, heads_weight_ref[...]) + heads_bias_ref[...]).astype(jnp.bfloat16)
    slots = lax.broadcasted_iota(jnp.int32, (length, length), 1)
    valid = slots < valid_ref[item]
    for pair in range(width // LANES):
        at = pair * LANES
        queries = heads_ref[:, at : at + LANES]
        keys = heads_ref[:, width + at : width + at + LANES]
        values = heads_ref[:, 2 * width + at : 2 * width + at + LANES]
        halves = []
        for side in range(2):
            head = 2 * pair + side
            scores = mult(half_of(queries, side), keys, RIGHT) * SCALE + bias_ref[head]
            scores = jnp.where(valid, scores, NEGATIVE)
            peak = jnp.max(scores, axis=-1, keepdims=True)
            powers = jnp.exp(scores - peak)
            probs = powers * (1.0 / jnp.sum(powers, axis=-1, keepdims=True))
            probs_ref[0, head] = probs
            halves.append(mult(probs.astype(jnp.bfloat16), values))
        mixed = join(*halves)
        mixed_ref[:, at : at + LANES] = mixed
        gains = head_gain_ref[:, at : at + LANES]
        scaled_ref[:, at : at + LANES] = (mixed * gains).astype(jnp.bfloat16)
    branch_ref[...] = mult(scaled_ref[...], merge_ref[...])


def attend(
    patches,
    valid,
    layer_input,
    own,
    other,
    gain,
    shift,
    heads_weight,
    heads_bias,
    bias,
    head_gain,
    merge,
):
    items = patches.shape[0]
    rows, model = layer_input.shape
    length = rows // items
    width = merge.shape[0]
    heads = bias.shape[0]
    out = lambda columns, kind: jax.ShapeDtypeStruct((rows, columns), kind)
    return pl.pallas_call(
        attend_kernel,
        grid_spec=pltpu.PrefetchScalarGridSpec(
            num_scalar_prefetch=2,
            grid=(items,),
            in_specs=[
                rows_of((length, model)),
                rows_of((length, model)),
                rows_of((length, model)),
                whole((1, model)),
                whole((1, model)),
                whole(heads_weight.shape),
                whole(heads_bias.shape),
                whole(bias.shape),
                whole(head_gain.shape),
                whole(merge.shape),
            ],
            out_specs=[
                rows_of((length, model)),
                rows_of((length, model)),
                rows_of((length, 3 * width)),
                pl.BlockSpec((1, heads, length, length), lambda item, *_: (item, 0, 0, 0)),
                rows_of((length, width)),
                rows_of((length, width)),
                rows_of((length, model)),
            ],
        ),
        out_shape=[
            out(model, jnp.float32),
            out(model, jnp.bfloat16),
            out(3 * width, jnp.bfloat16),
            jax.ShapeDtypeStruct((items, heads, length, length), jnp.float32),
            out(width, jnp.float32),
            out(width, jnp.bfloat16),
            out(model, jnp.float32),
        ],
        name="attend",
    )(
        patches,
        valid,
        layer_input,
        own,
        other,
        gain,
        shift,
        heads_weight,
        heads_bias,
        bias,
        head_gain,
        merge,
    )


def error_function(values):
    limited = jnp.clip(values, -3.7439211, 3.7439211)
    square = limited * limited
    top = jnp.full_like(square, 2.2905065861350646e-4)
    for factor in (
        3.4082910107109506e-3,
        5.0955695062380861e-2,
        1.8520832239976145e-1,
        1.128379143519084,
    ):
        top = top * square + factor
    bottom = jnp.full_like(square, -1.1791602954361697e-7)
    for factor in (
        2.3547966471313185e-5,
        1.0179625278914885e-3,
        1.4070470171167667e-2,
        1.1098505178285362e-1,
        4.9746925110067538e-1,
        1.0,
    ):
        bottom = bottom * square + factor
    return limited * top / bottom


def feed_kernel(
    valid_ref,
    hidden_ref,
    own_ref,
    other_ref,
    merge_bias_ref,
    gain_ref,
    shift_ref,
    expand_ref,
    expand_bias_ref,
    reduce_ref,
    upstream_ref,
    middle_ref,
    second_ref,
    active_ref,
    grad_expanded_ref,
    reduced_ref,
    grad_second_ref,
    grad_reduced_ref,
    expand_sum_ref,
    reduce_sum_ref,
):
    item = pl.program_id(0)
    length = hidden_ref.shape[0]
    start_sums(expand_sum_ref, reduce_sum_ref)
    middle = hidden_ref[...] + (own_ref[...] + other_ref[...]) + merge_bias_ref[...]
    middle_ref[...] = middle
    normal, _ = normed(middle)
    second = (normal * gain_ref[...] + shift_ref[...]).astype(jnp.bfloat16)
    second_ref[...] = second
    grad_result = upstream_ref[...].astype(jnp.float32) * before(length, valid_ref[item])
    reduce_sum_ref[...] += row_sum(grad_result)
    grad_reduced = grad_result.astype(jnp.bfloat16)
    grad_reduced_ref[...] = grad_reduced
    hidden_units = expand_ref.shape[1]
    part = hidden_units // 3
    reduced = None
    for at in range(0, hidden_units, part):
        span = slice(at, at + part)
        expanded = mult(second, expand_ref[:, span]) + expand_bias_ref[:, span]
        cumulative = 0.5 + 0.5 * error_function(expanded * 0.7071067811865476)
        active = (expanded * cumulative).astype(jnp.bfloat16)
        density = jnp.exp(expanded * expanded * -0.5) * 0.3989422804014327
        slope = cumulative + expanded * density
        active_ref[:, span] = active
        grad_active = mult(grad_reduced, reduce_ref[span, :], RIGHT)
        grad_expanded = (grad_active * slope).astype(jnp.bfloat16)
        grad_expanded_ref[:, span] = grad_expanded
        expand_sum_ref[:, span] += row_sum(grad_expanded.astype(jnp.float32))
        reduced_part = mult(active, reduce_ref[span, :])
        grad_part = mult(grad_expanded, expand_ref[:, span], RIGHT)
        if reduced is None:
            reduced, grad_second = reduced_part, grad_part
        else:
            reduced, grad_second = reduced + reduced_part, grad_second + grad_part
    reduced_ref[...] = reduced
    grad_second_ref[...] = grad_second


def feed(
    valid,
    hidden,
    own,
    other,
    merge_bias,
    gain,
    shift,
    expand,
    expand_bias,
    reduce_weight,
    upstream,
):
    items = valid.shape[0]
    rows, model = hidden.shape
    length = rows // items
    units = expand.shape[1]
    out = lambda columns, kind: jax.ShapeDtypeStruct((rows, columns), kind)
    model_rows = rows_of((length, model))
    unit_rows = rows_of((length, units))
    return pl.pallas_call(
        feed_kernel,
        grid_spec=pltpu.PrefetchScalarGridSpec(
            num_scalar_prefetch=1,
            grid=(items,),
            in_specs=[
                model_rows,
                model_rows,
                model_rows,
                whole((1, model)),
                whole((1, model)),
                whole((1, model)),
                whole(expand.shape),
                whole(expand_bias.shape),
                whole(reduce_weight.shape),
                model_rows,
            ],
            out_specs=[
                model_rows,
                model_rows,
                unit_rows,
                unit_rows,
                model_rows,
                model_rows,
                model_rows,
                whole((1, units)),
                whole((1, model)),
            ],
        ),
        out_shape=[
            out(model, jnp.float32),
            out(model, jnp.bfloat16),
            out(units, jnp.bfloat16),
            out(units, jnp.bfloat16),
            out(model, jnp.float32),
            out(model, jnp.float32),
            out(model, jnp.bfloat16),
            jax.ShapeDtypeStruct((1, units), jnp.float32),
            jax.ShapeDtypeStruct((1, model), jnp.float32),
        ],
        name="feed",
    )(
        valid,
        hidden,
        own,
        other,
        merge_bias,
        gain,
        shift,
        expand,
        expand_bias,
        reduce_weight,
        upstream,
    )


def attend_back_kernel(
    middle_ref,
    own_ref,
    other_ref,
    grad_reduced_ref,
    gain_ref,
    merge_ref,
    mixed_ref,
    head_gain_ref,
    probs_ref,
    heads_ref,
    heads_weight_ref,
    grad_middle_ref,
    grad_branch_ref,
    grad_heads_ref,
    grad_first_ref,
    gain_sum_ref,
    shift_sum_ref,
    merge_sum_ref,
    head_sum_ref,
    heads_sum_ref,
    table_ref,
    total_ref,
):
    item = pl.program_id(0)
    length = middle_ref.shape[0]
    width = mixed_ref.shape[1]
    start_sums(gain_sum_ref, shift_sum_ref, merge_sum_ref, head_sum_ref, heads_sum_ref, total_ref)
    normal, inverse = normed(middle_ref[...])
    grad_second = own_ref[...] + other_ref[...]
    gain_sum_ref[...] += row_sum(grad_second * normal)
    shift_sum_ref[...] += row_sum(grad_second)
    grad_middle = grad_reduced_ref[...].astype(jnp.float32) + norm_back(
        normal, inverse, grad_second, gain_ref[...]
    )
    grad_middle_ref[...] = grad_middle
    merge_sum_ref[...] += row_sum(grad_middle)
    grad_branch = grad_middle.astype(jnp.bfloat16)
    grad_branch_ref[...] = grad_branch
    grad_scaled = mult(grad_branch, merge_ref[...], RIGHT)
    head_sum_ref[...] += row_sum(grad_scaled * mixed_ref[...])
    grad_mixed = (grad_scaled * head_gain_ref[...]).astype(jnp.bfloat16)
    for pair in range(width // LANES):
        at = pair * LANES
        spans = [slice(k * width + at, k * width + at + LANES) for k in range(3)]
        queries, keys, values = (heads_ref[:, span] for span in spans)
        grads = grad_mixed[:, at : at + LANES]
        halves = []
        for side in range(2):
            head = 2 * pair + side
            probs = probs_ref[0, head]
            grad_values = mult(probs.astype(jnp.bfloat16), grads, LEFT)
            grad_probs = mult(half_of(grads, side), values, RIGHT)
            weighted = jnp.sum(probs * grad_probs, axis=-1, keepdims=True)
            grad_scores = (probs * (grad_probs - weighted)).astype(jnp.bfloat16)
            total_ref[head] += grad_scores.astype(jnp.float32)
            grad_queries = mult(grad_scores, keys) * SCALE
            grad_keys = mult(grad_scores, queries, LEFT) * SCALE
            halves.append((grad_queries, grad_keys, grad_values))
        for span, left, right in zip(spans, *halves):
            low = join(left, right).astype(jnp.bfloat16)
            grad_heads_ref[:, span] = low
            heads_sum_ref[:, span] += row_sum(low.astype(jnp.float32))
    grad_first_ref[...] = mult(grad_heads_ref[...], heads_weight_ref[...], RIGHT)

    @pl.when(item == pl.num_programs(0) - 1)
    def _():
        blank = jnp.zeros((length, length), jnp.float32)
        for head in range(total_ref.shape[0]):
            wide = jnp.concatenate([blank, total_ref[head]], axis=1)
            slots = length - 1 - lax.broadcasted_iota(jnp.int32, (length, length), 0)
            swap = jnp.where(lax.broadcasted_iota(jnp.int32, (length, length), 1) == slots, 1.0, 0.0)
            turned = lax.dot_general(
                swap,
                wide,
                (FULL, ((), ())),
                precision=lax.Precision.HIGHEST,
                preferred_element_type=jnp.float32,
            )
            turned = pltpu.roll(turned, length, 1, stride=1, stride_axis=0)
            table_ref[head : head + 1, :] = row_sum(turned)


def attend_back(
    items,
    middle,
    own,
    other,
    grad_reduced,
    gain,
    merge,
    mixed,
    head_gain,
    probs,
    heads_low,
    heads_weight,
):
    rows, model = middle.shape
    length = rows // items
    width = merge.shape[0]
    heads = probs.shape[1]
    out = lambda columns, kind: jax.ShapeDtypeStruct((rows, columns), kind)
    model_rows = rows_of((length, model))
    sums = lambda columns: jax.ShapeDtypeStruct((1, columns), jnp.float32)
    return pl.pallas_call(
        attend_back_kernel,
        grid_spec=pltpu.PrefetchScalarGridSpec(
            num_scalar_prefetch=0,
            grid=(items,),
            in_specs=[
                model_rows,
                model_rows,
                model_rows,
                model_rows,
                whole((1, model)),
                whole(merge.shape),
                rows_of((length, width)),
                whole(head_gain.shape),
                pl.BlockSpec((1, heads, length, length), lambda item, *_: (item, 0, 0, 0)),
                rows_of((length, 3 * width)),
                whole(heads_weight.shape),
            ],
            out_specs=[
                model_rows,
                model_rows,
                rows_of((length, 3 * width)),
                model_rows,
                whole((1, model)),
                whole((1, model)),
                whole((1, model)),
                whole((1, width)),
                whole((1, 3 * width)),
                whole((heads, 2 * length)),
            ],
            scratch_shapes=[pltpu.VMEM((heads, length, length), jnp.float32)],
        ),
        out_shape=[
            out(model, jnp.float32),
            out(model, jnp.bfloat16),
            out(3 * width, jnp.bfloat16),
            out(model, jnp.float32),
            sums(model),
            sums(model),
            sums(model),
            sums(width),
            sums(3 * width),
            jax.ShapeDtypeStruct((heads, 2 * length), jnp.float32),
        ],
        name="attend_back",
    )(
        middle,
        own,
        other,
        grad_reduced,
        gain,
        merge,
        mixed,
        head_gain,
        probs,
        heads_low,
        heads_weight,
    )


def stem_back_kernel(
    patches_ref,
    hidden_ref,
    own_ref,
    other_ref,
    grad_middle_ref,
    gain_ref,
    image_ref,
    features_ref,
    mean_ref,
    inverse_ref,
    input_grad_ref,
    grad_embedded_ref,
    grad_stem_ref,
    gain_sum_ref,
    shift_sum_ref,
    stem_gain_ref,
    stem_shift_ref,
):
    item = pl.program_id(0)
    length = hidden_ref.shape[0]
    start_sums(gain_sum_ref, shift_sum_ref, stem_gain_ref, stem_shift_ref)
    normal, inverse = normed(hidden_ref[...])
    grad_first = own_ref[...] + other_ref[...]
    gain_sum_ref[...] += row_sum(grad_first * normal)
    shift_sum_ref[...] += row_sum(grad_first)
    input_grad = grad_middle_ref[...] + norm_back(normal, inverse, grad_first, gain_ref[...])
    input_grad_ref[...] = input_grad
    mask = before(length, patches_ref[item])
    grad_embedded = (input_grad * mask).astype(jnp.bfloat16)
    grad_embedded_ref[...] = grad_embedded
    grad_stem = mult(grad_embedded, image_ref[...], RIGHT)
    grad_stem_ref[...] = grad_stem
    stem_hat = (features_ref[...].astype(jnp.float32) - mean_ref[...]) * inverse_ref[...]
    stem_shift_ref[...] += row_sum(grad_stem)
    stem_gain_ref[...] += row_sum(grad_stem * stem_hat)


def stem_back(
    patches, hidden, own, other, grad_middle, gain, image, features, mean, inverse
):
    items = patches.shape[0]
    rows, model = hidden.shape
    length = rows // items
    channels = features.shape[1]
    out = lambda columns, kind: jax.ShapeDtypeStruct((rows, columns), kind)
    model_rows = rows_of((length, model))
    channel_rows = rows_of((length, channels))
    sums = lambda columns: jax.ShapeDtypeStruct((1, columns), jnp.float32)
    return pl.pallas_call(
        stem_back_kernel,
        grid_spec=pltpu.PrefetchScalarGridSpec(
            num_scalar_prefetch=1,
            grid=(items,),
            in_specs=[
                model_rows,
                model_rows,
                model_rows,
                model_rows,
                whole((1, model)),
                whole(image.shape),
                channel_rows,
                whole((1, channels)),
                whole((1, channels)),
            ],
            out_specs=[
                model_rows,
                model_rows,
                channel_rows,
                whole((1, model)),
                whole((1, model)),
                whole((1, channels)),
                whole((1, channels)),
            ],
        ),
        out_shape=[
            out(model, jnp.float32),
            out(model, jnp.bfloat16),
            out(channels, jnp.float32),
            sums(model),
            sums(model),
            sums(channels),
            sums(channels),
        ],
        name="stem_back",
    )(patches, hidden, own, other, grad_middle, gain, image, features, mean, inverse)


def swap_core(values):
    count = lax.axis_size("tensor")
    return lax.ppermute(values, "tensor", [(core, core ^ 1) for core in range(count)])


def exchange(values, bit):
    count = lax.axis_size("dp")
    return lax.ppermute(values, "dp", [(rank, rank ^ (1 << bit)) for rank in range(count)])


def sum_by_doubling(values):
    for bit in range(lax.axis_size("dp").bit_length() - 1):
        values = values + exchange(values, bit)
    return values


def sum_by_halving(values, order):
    rank = lax.axis_index("dp")
    for bit in order:
        half = values.shape[0] // 2
        side = (rank >> bit) & 1
        sent = lax.dynamic_slice_in_dim(values, (1 - side) * half, half, 0)
        kept = lax.dynamic_slice_in_dim(values, side * half, half, 0)
        values = kept + exchange(sent, bit)
    for bit in reversed(order):
        side = (rank >> bit) & 1
        other = exchange(values, bit)
        values = jnp.where(
            side == 1, jnp.concatenate([other, values]), jnp.concatenate([values, other])
        )
    return values


def orders():
    bits = tuple(range(lax.axis_size("dp").bit_length() - 1))
    return bits, (bits[1], bits[0]) + bits[2:]


def pack(arrays):
    flat = jnp.concatenate([entry.reshape(-1) for entry in arrays])
    short = -flat.shape[0] % 1024
    return jnp.pad(flat, (0, short)).reshape(-1, 128)


def unpack(packed, arrays):
    flat, at, parts = packed.reshape(-1), 0, []
    for entry in arrays:
        parts.append(flat[at : at + entry.size].reshape(entry.shape))
        at += entry.size
    return parts


def local(
    layer_input,
    patch_features,
    bucket_ids,
    text_lengths,
    upstream,
    query_weight,
    key_weight,
    value_weight,
    merge_weight,
    query_bias,
    value_bias,
    merge_bias,
    head_gain,
    distance_table,
    first_gain,
    first_shift,
    second_gain,
    second_shift,
    expand_weight,
    expand_bias,
    reduce_weight,
    reduce_bias,
    image_weight,
    stem_gain,
    stem_shift,
):
    items = bucket_ids.shape[0]
    rows = layer_input.shape[0]
    length = rows // items
    heads = head_gain.shape[0]
    width = query_weight.shape[1]
    row = lambda vector: vector.reshape(1, -1)
    patches = PATCH_SMALL + (PATCH_LARGE - PATCH_SMALL) * bucket_ids
    valid = patches + text_lengths
    slots = jnp.arange(length, dtype=jnp.int32)
    patch_mask = (slots[None, :] < patches[:, None]).astype(jnp.float32).reshape(rows)
    features = patch_features.astype(jnp.float32)
    masked = features * patch_mask[:, None]
    feature_sum, square_sum, count = sum_by_doubling(
        jnp.stack(
            [
                jnp.sum(masked, axis=0),
                jnp.sum(masked * features, axis=0),
                jnp.full((features.shape[1],), jnp.sum(patch_mask)),
            ]
        )
    )
    bias = distance_bias(distance_table, length)
    heads_weight = jnp.concatenate([query_weight, key_weight, value_weight], axis=1)
    heads_bias = row(jnp.concatenate([query_bias, jnp.zeros_like(query_bias), value_bias]))
    head_gains = row(jnp.repeat(head_gain, HEAD_DIM))
    stem_mean = feature_sum / count
    stem_inverse = lax.rsqrt(square_sum / count - stem_mean * stem_mean + EPSILON)
    stem_hat = (features - stem_mean) * stem_inverse
    stem_low = (stem_hat * stem_gain + stem_shift).astype(jnp.bfloat16)
    embedded = mult(stem_low, image_weight)
    hidden, first_low, heads_low, probs, mixed, scaled_low, branch = attend(
        patches,
        valid,
        layer_input,
        embedded,
        swap_core(embedded),
        row(first_gain),
        row(first_shift),
        heads_weight,
        heads_bias,
        bias,
        head_gains,
        merge_weight,
    )
    (
        middle,
        second_low,
        active_low,
        grad_expanded_low,
        reduced,
        grad_second,
        grad_reduced_low,
        grad_expand_bias,
        grad_reduce_bias,
    ) = feed(
        valid,
        hidden,
        branch,
        swap_core(branch),
        row(merge_bias),
        row(second_gain),
        row(second_shift),
        expand_weight,
        row(expand_bias),
        reduce_weight,
        upstream,
    )
    grad_reduce_weight = mult(active_low, grad_reduced_low, LEFT)
    grad_expand_weight = mult(second_low, grad_expanded_low, LEFT)
    block_output = (middle + (reduced + swap_core(reduced)) + reduce_bias).astype(jnp.bfloat16)
    (
        grad_middle,
        grad_branch_low,
        grad_heads_low,
        grad_first,
        grad_second_gain,
        grad_second_shift,
        grad_merge_bias,
        head_sums,
        heads_sums,
        grad_table,
    ) = attend_back(
        items,
        middle,
        grad_second,
        swap_core(grad_second),
        grad_reduced_low,
        row(second_gain),
        merge_weight,
        mixed,
        head_gains,
        probs,
        heads_low,
        heads_weight,
    )
    grad_merge_weight = mult(scaled_low, grad_branch_low, LEFT)
    grad_heads_weight = mult(first_low, grad_heads_low, LEFT)
    (
        input_grad,
        grad_embedded_low,
        grad_stem,
        grad_first_gain,
        grad_first_shift,
        gain_local,
        shift_local,
    ) = stem_back(
        patches,
        hidden,
        grad_first,
        swap_core(grad_first),
        grad_middle,
        row(first_gain),
        image_weight,
        patch_features,
        row(stem_mean),
        row(stem_inverse),
    )
    grad_image_weight = mult(stem_low, grad_embedded_low, LEFT)
    first_order, second_order = orders()
    grad_reduce_weight = sum_by_halving(grad_reduce_weight, first_order)
    grad_expand_weight = sum_by_halving(grad_expand_weight, second_order)
    merge_rows = grad_merge_weight.shape[0]
    row_weights = sum_by_halving(
        jnp.concatenate([grad_merge_weight, grad_image_weight]), second_order
    )
    grad_merge_weight, grad_image_weight = row_weights[:merge_rows], row_weights[merge_rows:]
    grad_heads_weight = sum_by_halving(grad_heads_weight, first_order)
    small = (
        heads_sums,
        grad_merge_bias,
        jnp.sum(head_sums.reshape(heads, HEAD_DIM), axis=1),
        grad_table[:, : distance_table.shape[1]],
        grad_first_gain,
        grad_first_shift,
        grad_second_gain,
        grad_second_shift,
        grad_expand_bias,
        grad_reduce_bias,
        gain_local,
        shift_local,
    )
    (
        heads_sums,
        grad_merge_bias,
        grad_head_gain,
        grad_distance_table,
        grad_first_gain,
        grad_first_shift,
        grad_second_gain,
        grad_second_shift,
        grad_expand_bias,
        grad_reduce_bias,
        grad_stem_gain,
        grad_stem_shift,
    ) = unpack(sum_by_doubling(pack(small)), small)
    patch_grad = (
        patch_mask[:, None]
        * stem_inverse
        * stem_gain
        * (grad_stem - grad_stem_shift / count - stem_hat * grad_stem_gain / count)
    )
    return (
        block_output,
        input_grad,
        patch_grad,
        grad_heads_weight[:, :width],
        grad_heads_weight[:, width : 2 * width],
        grad_heads_weight[:, 2 * width :],
        grad_merge_weight,
        heads_sums[0, :width],
        heads_sums[0, 2 * width :],
        grad_merge_bias[0],
        grad_head_gain,
        grad_distance_table,
        grad_first_gain[0],
        grad_first_shift[0],
        grad_second_gain[0],
        grad_second_shift[0],
        grad_expand_weight,
        grad_expand_bias[0],
        grad_reduce_weight,
        grad_reduce_bias[0],
        grad_image_weight,
        grad_stem_gain[0],
        grad_stem_shift[0],
    )


def solution(mesh):
    in_specs = (
        P("dp", None),
        P("dp", "tensor"),
        P("dp"),
        P("dp"),
        P("dp", None),
        P(None, "tensor"),
        P(None, "tensor"),
        P(None, "tensor"),
        P("tensor", None),
        P("tensor"),
        P("tensor"),
        P(),
        P("tensor"),
        P("tensor", None),
        P(),
        P(),
        P(),
        P(),
        P(None, "tensor"),
        P("tensor"),
        P("tensor", None),
        P(),
        P("tensor", None),
        P("tensor"),
        P("tensor"),
    )
    out_specs = (
        P("dp", None),
        P("dp", None),
        P("dp", "tensor"),
        P(None, "tensor"),
        P(None, "tensor"),
        P(None, "tensor"),
        P("tensor", None),
        P("tensor"),
        P("tensor"),
        P(),
        P("tensor"),
        P("tensor", None),
        P(),
        P(),
        P(),
        P(),
        P(None, "tensor"),
        P("tensor"),
        P("tensor", None),
        P(),
        P("tensor", None),
        P("tensor"),
        P("tensor"),
    )
    return jax.shard_map(local, mesh=mesh, in_specs=in_specs, out_specs=out_specs, check_vma=False)
```

```python
from functools import partial

import jax
import jax.numpy as jnp
from jax import lax
from jax.experimental import pallas as pl
from jax.experimental.pallas import tpu as pltpu
from jax.sharding import PartitionSpec as P

HEAD_DIM = 64
PATCH_SMALL = 64
PATCH_LARGE = 225
EPSILON = 1e-05
NEGATIVE = -1e30
SCALE = HEAD_DIM ** (-0.5)
LANES = 128
FULL = ((1,), (0,))
RIGHT = ((1,), (1,))
LEFT = ((0,), (0,))
SCHEDULE = " ".join(
    (
        "R a R E",
        "h b R E",
        "i R H E",
        "R E R w",
        "H E o s",
        "R H s R",
        "s H E H",
        "s E R E",
        "H H p H",
        "E H",
    )
)


def cost(micros):
    return pl.CostEstimate(
        flops=micros * 10**9, transcendentals=0, bytes_accessed=micros * 3 * 10**6
    )


def mult(left, right, dims=FULL):
    return lax.dot_general(left, right, (dims, ((), ())), preferred_element_type=jnp.float32)


def rows_of(length):
    return pl.BlockSpec((length[0], length[1]), lambda item, *_: (item, 0))


def whole(shape):
    return pl.BlockSpec(shape, lambda item, *_: (0,) * len(shape))


def normed(values):
    centered = values - jnp.mean(values, axis=-1, keepdims=True)
    inverse = lax.rsqrt(jnp.mean(centered * centered, axis=-1, keepdims=True) + EPSILON)
    return centered * inverse, inverse


def before(length, limit):
    slots = lax.broadcasted_iota(jnp.int32, (length, 1), 0)
    return jnp.where(slots < limit, 1.0, 0.0).astype(jnp.float32)


def norm_back(normal, inverse, grad, gain):
    scaled = grad * gain
    first = jnp.mean(scaled, axis=-1, keepdims=True)
    second = jnp.mean(scaled * normal, axis=-1, keepdims=True)
    return (scaled - first - normal * second) * inverse


def row_sum(values):
    return jnp.sum(values, axis=0, keepdims=True)


def start_sums(*refs):
    @pl.when(pl.program_id(0) == 0)
    def _():
        for ref in refs:
            ref[...] = jnp.zeros(ref.shape, ref.dtype)


def bias_kernel(table_ref, out_ref):
    length = out_ref.shape[1]
    for head in range(out_ref.shape[0]):
        rows = jnp.broadcast_to(table_ref[head : head + 1, :], (length, 2 * length))
        turned = pltpu.roll(rows, length + 1, 1, stride=1, stride_axis=0)
        out_ref[head] = turned[:, :length]


def distance_bias(table, length):
    heads = table.shape[0]
    padded = jnp.pad(table, ((0, 0), (0, 2 * length - table.shape[1])))
    return pl.pallas_call(
        bias_kernel,
        out_shape=jax.ShapeDtypeStruct((heads, length, length), jnp.float32),
        cost_estimate=cost(2),
        name="distance_bias",
    )(padded)


def half_of(pair, side):
    lanes = lax.broadcasted_iota(jnp.int32, pair.shape, 1)
    keep = lanes < HEAD_DIM if side == 0 else lanes >= HEAD_DIM
    return jnp.where(keep, pair, jnp.zeros_like(pair))


def join(left, right):
    lanes = lax.broadcasted_iota(jnp.int32, left.shape, 1)
    return jnp.where(lanes < HEAD_DIM, left, right)


def attend_kernel(
    patches_ref,
    valid_ref,
    input_ref,
    own_ref,
    other_ref,
    gain_ref,
    shift_ref,
    heads_weight_ref,
    heads_bias_ref,
    bias_ref,
    head_gain_ref,
    merge_ref,
    hidden_ref,
    first_ref,
    heads_ref,
    probs_ref,
    mixed_ref,
    scaled_ref,
    branch_ref,
):
    item = pl.program_id(0)
    length = input_ref.shape[0]
    width = mixed_ref.shape[1]
    mask = before(length, patches_ref[item])
    hidden = input_ref[...].astype(jnp.float32) + mask * (own_ref[...] + other_ref[...])
    hidden_ref[...] = hidden
    normal, _ = normed(hidden)
    first = (normal * gain_ref[...] + shift_ref[...]).astype(jnp.bfloat16)
    first_ref[...] = first
    heads_ref[...] = (mult(first, heads_weight_ref[...]) + heads_bias_ref[...]).astype(jnp.bfloat16)
    slots = lax.broadcasted_iota(jnp.int32, (length, length), 1)
    valid = slots < valid_ref[item]
    for pair in range(width // LANES):
        at = pair * LANES
        queries = heads_ref[:, at : at + LANES]
        keys = heads_ref[:, width + at : width + at + LANES]
        values = heads_ref[:, 2 * width + at : 2 * width + at + LANES]
        halves = []
        for side in range(2):
            head = 2 * pair + side
            scores = mult(half_of(queries, side), keys, RIGHT) * SCALE + bias_ref[head]
            scores = jnp.where(valid, scores, NEGATIVE)
            peak = jnp.max(scores, axis=-1, keepdims=True)
            powers = jnp.exp(scores - peak)
            probs = powers * (1.0 / jnp.sum(powers, axis=-1, keepdims=True))
            probs_ref[0, head] = probs
            halves.append(mult(probs.astype(jnp.bfloat16), values))
        mixed = join(*halves)
        mixed_ref[:, at : at + LANES] = mixed
        gains = head_gain_ref[:, at : at + LANES]
        scaled_ref[:, at : at + LANES] = (mixed * gains).astype(jnp.bfloat16)
    branch_ref[...] = mult(scaled_ref[...], merge_ref[...])


def attend(
    patches,
    valid,
    layer_input,
    own,
    other,
    gain,
    shift,
    heads_weight,
    heads_bias,
    bias,
    head_gain,
    merge,
):
    items = patches.shape[0]
    rows, model = layer_input.shape
    length = rows // items
    width = merge.shape[0]
    heads = bias.shape[0]
    out = lambda columns, kind: jax.ShapeDtypeStruct((rows, columns), kind)
    return pl.pallas_call(
        attend_kernel,
        grid_spec=pltpu.PrefetchScalarGridSpec(
            num_scalar_prefetch=2,
            grid=(items,),
            in_specs=[
                rows_of((length, model)),
                rows_of((length, model)),
                rows_of((length, model)),
                whole((1, model)),
                whole((1, model)),
                whole(heads_weight.shape),
                whole(heads_bias.shape),
                whole(bias.shape),
                whole(head_gain.shape),
                whole(merge.shape),
            ],
            out_specs=[
                rows_of((length, model)),
                rows_of((length, model)),
                rows_of((length, 3 * width)),
                pl.BlockSpec((1, heads, length, length), lambda item, *_: (item, 0, 0, 0)),
                rows_of((length, width)),
                rows_of((length, width)),
                rows_of((length, model)),
            ],
        ),
        out_shape=[
            out(model, jnp.float32),
            out(model, jnp.bfloat16),
            out(3 * width, jnp.bfloat16),
            jax.ShapeDtypeStruct((items, heads, length, length), jnp.float32),
            out(width, jnp.float32),
            out(width, jnp.bfloat16),
            out(model, jnp.float32),
        ],
        cost_estimate=cost(15),
        name="attend",
    )(
        patches,
        valid,
        layer_input,
        own,
        other,
        gain,
        shift,
        heads_weight,
        heads_bias,
        bias,
        head_gain,
        merge,
    )


def error_function(values):
    limited = jnp.clip(values, -3.7439211, 3.7439211)
    square = limited * limited
    top = jnp.full_like(square, 2.2905065861350646e-4)
    for factor in (
        3.4082910107109506e-3,
        5.0955695062380861e-2,
        1.8520832239976145e-1,
        1.128379143519084,
    ):
        top = top * square + factor
    bottom = jnp.full_like(square, -1.1791602954361697e-7)
    for factor in (
        2.3547966471313185e-5,
        1.0179625278914885e-3,
        1.4070470171167667e-2,
        1.1098505178285362e-1,
        4.9746925110067538e-1,
        1.0,
    ):
        bottom = bottom * square + factor
    return limited * top / bottom


def feed_kernel(
    valid_ref,
    hidden_ref,
    own_ref,
    other_ref,
    merge_bias_ref,
    gain_ref,
    shift_ref,
    expand_ref,
    expand_bias_ref,
    reduce_ref,
    upstream_ref,
    middle_ref,
    second_ref,
    active_ref,
    grad_expanded_ref,
    reduced_ref,
    grad_second_ref,
    grad_reduced_ref,
    expand_sum_ref,
    reduce_sum_ref,
):
    item = pl.program_id(0)
    length = hidden_ref.shape[0]
    start_sums(expand_sum_ref, reduce_sum_ref)
    middle = hidden_ref[...] + (own_ref[...] + other_ref[...]) + merge_bias_ref[...]
    middle_ref[...] = middle
    normal, _ = normed(middle)
    second = (normal * gain_ref[...] + shift_ref[...]).astype(jnp.bfloat16)
    second_ref[...] = second
    grad_result = upstream_ref[...].astype(jnp.float32) * before(length, valid_ref[item])
    reduce_sum_ref[...] += row_sum(grad_result)
    grad_reduced = grad_result.astype(jnp.bfloat16)
    grad_reduced_ref[...] = grad_reduced
    hidden_units = expand_ref.shape[1]
    part = hidden_units // 3
    reduced = None
    for at in range(0, hidden_units, part):
        span = slice(at, at + part)
        expanded = mult(second, expand_ref[:, span]) + expand_bias_ref[:, span]
        cumulative = 0.5 + 0.5 * error_function(expanded * 0.7071067811865476)
        active = (expanded * cumulative).astype(jnp.bfloat16)
        density = jnp.exp(expanded * expanded * -0.5) * 0.3989422804014327
        slope = cumulative + expanded * density
        active_ref[:, span] = active
        grad_active = mult(grad_reduced, reduce_ref[span, :], RIGHT)
        grad_expanded = (grad_active * slope).astype(jnp.bfloat16)
        grad_expanded_ref[:, span] = grad_expanded
        expand_sum_ref[:, span] += row_sum(grad_expanded.astype(jnp.float32))
        reduced_part = mult(active, reduce_ref[span, :])
        grad_part = mult(grad_expanded, expand_ref[:, span], RIGHT)
        if reduced is None:
            reduced, grad_second = reduced_part, grad_part
        else:
            reduced, grad_second = reduced + reduced_part, grad_second + grad_part
    reduced_ref[...] = reduced
    grad_second_ref[...] = grad_second


def feed(
    valid,
    hidden,
    own,
    other,
    merge_bias,
    gain,
    shift,
    expand,
    expand_bias,
    reduce_weight,
    upstream,
):
    items = valid.shape[0]
    rows, model = hidden.shape
    length = rows // items
    units = expand.shape[1]
    out = lambda columns, kind: jax.ShapeDtypeStruct((rows, columns), kind)
    model_rows = rows_of((length, model))
    unit_rows = rows_of((length, units))
    return pl.pallas_call(
        feed_kernel,
        grid_spec=pltpu.PrefetchScalarGridSpec(
            num_scalar_prefetch=1,
            grid=(items,),
            in_specs=[
                model_rows,
                model_rows,
                model_rows,
                whole((1, model)),
                whole((1, model)),
                whole((1, model)),
                whole(expand.shape),
                whole(expand_bias.shape),
                whole(reduce_weight.shape),
                model_rows,
            ],
            out_specs=[
                model_rows,
                model_rows,
                unit_rows,
                unit_rows,
                model_rows,
                model_rows,
                model_rows,
                whole((1, units)),
                whole((1, model)),
            ],
        ),
        out_shape=[
            out(model, jnp.float32),
            out(model, jnp.bfloat16),
            out(units, jnp.bfloat16),
            out(units, jnp.bfloat16),
            out(model, jnp.float32),
            out(model, jnp.float32),
            out(model, jnp.bfloat16),
            jax.ShapeDtypeStruct((1, units), jnp.float32),
            jax.ShapeDtypeStruct((1, model), jnp.float32),
        ],
        cost_estimate=cost(23),
        name="feed",
    )(
        valid,
        hidden,
        own,
        other,
        merge_bias,
        gain,
        shift,
        expand,
        expand_bias,
        reduce_weight,
        upstream,
    )


def attend_back_kernel(
    middle_ref,
    own_ref,
    other_ref,
    grad_reduced_ref,
    gain_ref,
    merge_ref,
    mixed_ref,
    head_gain_ref,
    probs_ref,
    heads_ref,
    heads_weight_ref,
    grad_middle_ref,
    grad_branch_ref,
    grad_heads_ref,
    grad_first_ref,
    gain_sum_ref,
    shift_sum_ref,
    merge_sum_ref,
    head_sum_ref,
    heads_sum_ref,
    table_ref,
    total_ref,
):
    item = pl.program_id(0)
    length = middle_ref.shape[0]
    width = mixed_ref.shape[1]
    start_sums(gain_sum_ref, shift_sum_ref, merge_sum_ref, head_sum_ref, heads_sum_ref, total_ref)
    normal, inverse = normed(middle_ref[...])
    grad_second = own_ref[...] + other_ref[...]
    gain_sum_ref[...] += row_sum(grad_second * normal)
    shift_sum_ref[...] += row_sum(grad_second)
    grad_middle = grad_reduced_ref[...].astype(jnp.float32) + norm_back(
        normal, inverse, grad_second, gain_ref[...]
    )
    grad_middle_ref[...] = grad_middle
    merge_sum_ref[...] += row_sum(grad_middle)
    grad_branch = grad_middle.astype(jnp.bfloat16)
    grad_branch_ref[...] = grad_branch
    grad_scaled = mult(grad_branch, merge_ref[...], RIGHT)
    head_sum_ref[...] += row_sum(grad_scaled * mixed_ref[...])
    grad_mixed = (grad_scaled * head_gain_ref[...]).astype(jnp.bfloat16)
    for pair in range(width // LANES):
        at = pair * LANES
        spans = [slice(k * width + at, k * width + at + LANES) for k in range(3)]
        queries, keys, values = (heads_ref[:, span] for span in spans)
        grads = grad_mixed[:, at : at + LANES]
        halves = []
        for side in range(2):
            head = 2 * pair + side
            probs = probs_ref[0, head]
            grad_values = mult(probs.astype(jnp.bfloat16), grads, LEFT)
            grad_probs = mult(half_of(grads, side), values, RIGHT)
            weighted = jnp.sum(probs * grad_probs, axis=-1, keepdims=True)
            grad_scores = (probs * (grad_probs - weighted)).astype(jnp.bfloat16)
            total_ref[head] += grad_scores.astype(jnp.float32)
            grad_queries = mult(grad_scores, keys) * SCALE
            grad_keys = mult(grad_scores, queries, LEFT) * SCALE
            halves.append((grad_queries, grad_keys, grad_values))
        for span, left, right in zip(spans, *halves):
            low = join(left, right).astype(jnp.bfloat16)
            grad_heads_ref[:, span] = low
            heads_sum_ref[:, span] += row_sum(low.astype(jnp.float32))
    grad_first_ref[...] = mult(grad_heads_ref[...], heads_weight_ref[...], RIGHT)

    @pl.when(item == pl.num_programs(0) - 1)
    def _():
        blank = jnp.zeros((length, length), jnp.float32)
        for head in range(total_ref.shape[0]):
            wide = jnp.concatenate([blank, total_ref[head]], axis=1)
            slots = length - 1 - lax.broadcasted_iota(jnp.int32, (length, length), 0)
            swap = jnp.where(lax.broadcasted_iota(jnp.int32, (length, length), 1) == slots, 1.0, 0.0)
            turned = lax.dot_general(
                swap,
                wide,
                (FULL, ((), ())),
                precision=lax.Precision.HIGHEST,
                preferred_element_type=jnp.float32,
            )
            turned = pltpu.roll(turned, length, 1, stride=1, stride_axis=0)
            table_ref[head : head + 1, :] = row_sum(turned)


def attend_back(
    items,
    middle,
    own,
    other,
    grad_reduced,
    gain,
    merge,
    mixed,
    head_gain,
    probs,
    heads_low,
    heads_weight,
):
    rows, model = middle.shape
    length = rows // items
    width = merge.shape[0]
    heads = probs.shape[1]
    out = lambda columns, kind: jax.ShapeDtypeStruct((rows, columns), kind)
    model_rows = rows_of((length, model))
    sums = lambda columns: jax.ShapeDtypeStruct((1, columns), jnp.float32)
    return pl.pallas_call(
        attend_back_kernel,
        grid_spec=pltpu.PrefetchScalarGridSpec(
            num_scalar_prefetch=0,
            grid=(items,),
            in_specs=[
                model_rows,
                model_rows,
                model_rows,
                model_rows,
                whole((1, model)),
                whole(merge.shape),
                rows_of((length, width)),
                whole(head_gain.shape),
                pl.BlockSpec((1, heads, length, length), lambda item, *_: (item, 0, 0, 0)),
                rows_of((length, 3 * width)),
                whole(heads_weight.shape),
            ],
            out_specs=[
                model_rows,
                model_rows,
                rows_of((length, 3 * width)),
                model_rows,
                whole((1, model)),
                whole((1, model)),
                whole((1, model)),
                whole((1, width)),
                whole((1, 3 * width)),
                whole((heads, 2 * length)),
            ],
            scratch_shapes=[pltpu.VMEM((heads, length, length), jnp.float32)],
        ),
        out_shape=[
            out(model, jnp.float32),
            out(model, jnp.bfloat16),
            out(3 * width, jnp.bfloat16),
            out(model, jnp.float32),
            sums(model),
            sums(model),
            sums(model),
            sums(width),
            sums(3 * width),
            jax.ShapeDtypeStruct((heads, 2 * length), jnp.float32),
        ],
        cost_estimate=cost(24),
        name="attend_back",
    )(
        middle,
        own,
        other,
        grad_reduced,
        gain,
        merge,
        mixed,
        head_gain,
        probs,
        heads_low,
        heads_weight,
    )


def stem_back_kernel(
    patches_ref,
    hidden_ref,
    own_ref,
    other_ref,
    grad_middle_ref,
    gain_ref,
    image_ref,
    features_ref,
    mean_ref,
    inverse_ref,
    input_grad_ref,
    grad_embedded_ref,
    grad_stem_ref,
    gain_sum_ref,
    shift_sum_ref,
    stem_gain_ref,
    stem_shift_ref,
):
    item = pl.program_id(0)
    length = hidden_ref.shape[0]
    start_sums(gain_sum_ref, shift_sum_ref, stem_gain_ref, stem_shift_ref)
    normal, inverse = normed(hidden_ref[...])
    grad_first = own_ref[...] + other_ref[...]
    gain_sum_ref[...] += row_sum(grad_first * normal)
    shift_sum_ref[...] += row_sum(grad_first)
    input_grad = grad_middle_ref[...] + norm_back(normal, inverse, grad_first, gain_ref[...])
    input_grad_ref[...] = input_grad
    mask = before(length, patches_ref[item])
    grad_embedded = (input_grad * mask).astype(jnp.bfloat16)
    grad_embedded_ref[...] = grad_embedded
    grad_stem = mult(grad_embedded, image_ref[...], RIGHT)
    grad_stem_ref[...] = grad_stem
    stem_hat = (features_ref[...].astype(jnp.float32) - mean_ref[...]) * inverse_ref[...]
    stem_shift_ref[...] += row_sum(grad_stem)
    stem_gain_ref[...] += row_sum(grad_stem * stem_hat)


def stem_back(
    patches, hidden, own, other, grad_middle, gain, image, features, mean, inverse
):
    items = patches.shape[0]
    rows, model = hidden.shape
    length = rows // items
    channels = features.shape[1]
    out = lambda columns, kind: jax.ShapeDtypeStruct((rows, columns), kind)
    model_rows = rows_of((length, model))
    channel_rows = rows_of((length, channels))
    sums = lambda columns: jax.ShapeDtypeStruct((1, columns), jnp.float32)
    return pl.pallas_call(
        stem_back_kernel,
        grid_spec=pltpu.PrefetchScalarGridSpec(
            num_scalar_prefetch=1,
            grid=(items,),
            in_specs=[
                model_rows,
                model_rows,
                model_rows,
                model_rows,
                whole((1, model)),
                whole(image.shape),
                channel_rows,
                whole((1, channels)),
                whole((1, channels)),
            ],
            out_specs=[
                model_rows,
                model_rows,
                channel_rows,
                whole((1, model)),
                whole((1, model)),
                whole((1, channels)),
                whole((1, channels)),
            ],
        ),
        out_shape=[
            out(model, jnp.float32),
            out(model, jnp.bfloat16),
            out(channels, jnp.float32),
            sums(model),
            sums(model),
            sums(channels),
            sums(channels),
        ],
        cost_estimate=cost(10),
        name="stem_back",
    )(patches, hidden, own, other, grad_middle, gain, image, features, mean, inverse)


def swap_core(values):
    count = lax.axis_size("tensor")
    return lax.ppermute(values, "tensor", [(core, core ^ 1) for core in range(count)])


def exchange(values, bit):
    count = lax.axis_size("dp")
    return lax.ppermute(values, "dp", [(rank, rank ^ (1 << bit)) for rank in range(count)])


def sum_by_doubling(values):
    for bit in range(lax.axis_size("dp").bit_length() - 1):
        values = values + exchange(values, bit)
    return values


class Chain:
    def __init__(self):
        self.token = ()

    def enter(self, *arrays):
        held = lax.optimization_barrier((*self.token, *arrays))
        return held[len(self.token) :]

    def leave(self, *arrays):
        self.token = arrays
        return arrays


def cut(values, side):
    half = values.shape[1] // 2
    return lax.dynamic_slice_in_dim(values, side * half, half, 1)


def spread(side, mine, other):
    return jnp.where(
        side == 1,
        jnp.concatenate([other, mine], axis=1),
        jnp.concatenate([mine, other], axis=1),
    )


def regroup(arrays, count):
    if len(arrays) == count:
        return list(arrays)
    if count == 1:
        return [jnp.concatenate(arrays, axis=0)]
    return list(jnp.split(arrays[0], count, axis=0))


class Stream:
    def __init__(self, chain):
        bits = lax.axis_size("dp").bit_length() - 1
        self.chain = chain
        self.rank = lax.axis_index("dp")
        self.plan = ((0, 1), (1, 0)) + tuple((bit,) for bit in range(2, bits))
        self.stage = 0

    def bits(self, stage):
        steps = self.plan + self.plan[::-1]
        return steps[stage]

    def sides(self, stage):
        return [(self.rank >> bit) & 1 for bit in self.bits(stage)]

    def send(self, arrays):
        arrays = self.chain.leave(*arrays)
        self.flight = [exchange(array, bit) for array, bit in zip(arrays, self.bits(self.stage))]

    def launch(self, *parts):
        sides = self.sides(0)
        self.send([part(1 - side) for part, side in zip(parts, sides)])
        self.kept = [part(side) for part, side in zip(parts, sides)]

    def step(self):
        steps = len(self.plan)
        if self.stage == 2 * steps:
            return
        held = self.chain.enter(*self.flight)
        self.stage += 1
        if self.stage < steps:
            count = len(self.bits(self.stage))
            kept, held = regroup(self.kept, count), regroup(held, count)
            sides = self.sides(self.stage)
            pairs = list(zip(kept, held, sides))
            self.send([cut(mine, 1 - side) + cut(other, 1 - side) for mine, other, side in pairs])
            self.kept = [cut(mine, side) + cut(other, side) for mine, other, side in pairs]
        elif self.stage == steps:
            self.values = [mine + other for mine, other in zip(self.kept, held)]
            self.send(self.values)
        else:
            sides = self.sides(self.stage - 1)
            self.last = list(zip(sides, self.values, held))
            if self.stage < 2 * steps:
                values = [spread(*entry) for entry in self.last]
                self.values = regroup(values, len(self.bits(self.stage)))
                self.send(self.values)
            else:
                self.chain.leave(*held)

    def finish(self):
        while self.stage < 2 * len(self.plan):
            self.step()
        return self.last


def piece(entry, start, stop):
    side, mine, other = entry
    whole_rows = spread(side, mine[start:stop], other[start:stop])
    return whole_rows.reshape(-1, whole_rows.shape[2])


def pack(arrays):
    flat = jnp.concatenate([entry.reshape(-1) for entry in arrays])
    short = -flat.shape[0] % 1024
    return jnp.pad(flat, (0, short)).reshape(-1, 128)


def unpack(packed, arrays):
    flat, at, parts = packed.reshape(-1), 0, []
    for entry in arrays:
        parts.append(flat[at : at + entry.size].reshape(entry.shape))
        at += entry.size
    return parts


def local(
    layer_input,
    patch_features,
    bucket_ids,
    text_lengths,
    upstream,
    query_weight,
    key_weight,
    value_weight,
    merge_weight,
    query_bias,
    value_bias,
    merge_bias,
    head_gain,
    distance_table,
    first_gain,
    first_shift,
    second_gain,
    second_shift,
    expand_weight,
    expand_bias,
    reduce_weight,
    reduce_bias,
    image_weight,
    stem_gain,
    stem_shift,
):
    items = bucket_ids.shape[0]
    rows = layer_input.shape[0]
    length = rows // items
    heads = head_gain.shape[0]
    width = query_weight.shape[1]
    row = lambda vector: vector.reshape(1, -1)
    patches = PATCH_SMALL + (PATCH_LARGE - PATCH_SMALL) * bucket_ids
    valid = patches + text_lengths
    slots = jnp.arange(length, dtype=jnp.int32)
    patch_mask = (slots[None, :] < patches[:, None]).astype(jnp.float32).reshape(rows)
    features = patch_features.astype(jnp.float32)
    masked = features * patch_mask[:, None]
    feature_sum, square_sum, count = sum_by_doubling(
        jnp.stack(
            [
                jnp.sum(masked, axis=0),
                jnp.sum(masked * features, axis=0),
                jnp.full((features.shape[1],), jnp.sum(patch_mask)),
            ]
        )
    )
    bias = distance_bias(distance_table, length)
    heads_weight = jnp.concatenate([query_weight, key_weight, value_weight], axis=1)
    heads_bias = row(jnp.concatenate([query_bias, jnp.zeros_like(query_bias), value_bias]))
    head_gains = row(jnp.repeat(head_gain, HEAD_DIM))
    stem_mean = feature_sum / count
    stem_inverse = lax.rsqrt(square_sum / count - stem_mean * stem_mean + EPSILON)
    stem_hat = (features - stem_mean) * stem_inverse
    stem_low = (stem_hat * stem_gain + stem_shift).astype(jnp.bfloat16)
    embedded = mult(stem_low, image_weight)
    hidden, first_low, heads_low, probs, mixed, scaled_low, branch = attend(
        patches,
        valid,
        layer_input,
        embedded,
        swap_core(embedded),
        row(first_gain),
        row(first_shift),
        heads_weight,
        heads_bias,
        bias,
        head_gains,
        merge_weight,
    )
    (
        middle,
        second_low,
        active_low,
        grad_expanded_low,
        reduced,
        grad_second,
        grad_reduced_low,
        grad_expand_bias,
        grad_reduce_bias,
    ) = feed(
        valid,
        hidden,
        branch,
        swap_core(branch),
        row(merge_bias),
        row(second_gain),
        row(second_shift),
        expand_weight,
        row(expand_bias),
        reduce_weight,
        upstream,
    )
    chain = Chain()
    reduces, expands, others = Stream(chain), Stream(chain), Stream(chain)
    streams = {"R": reduces, "E": expands, "H": others}
    slot = 256
    state = {}

    def reduce_part(at, size):
        def part(side):
            units = lax.dynamic_slice_in_dim(active_low, at + side * (size // 2), size // 2, 1)
            return mult(units, grad_reduced_low, LEFT)[None]

        return part

    def expand_part(at, size):
        def part(side):
            half = second_low.shape[1] // 2
            columns = lax.dynamic_slice_in_dim(state["second"], side * half, half, 1)
            return mult(columns, grad_expanded_low[:, at : at + size], LEFT)[None]

        return part

    def launch_reduces():
        size = active_low.shape[1] // 2
        reduces.launch(reduce_part(0, size), reduce_part(size, size))

    def launch_expands():
        (state["second"],) = chain.enter(second_low)
        size = grad_expanded_low.shape[1] // 2
        expands.launch(expand_part(0, size), expand_part(size, size))

    def run_attend_back():
        (other,) = chain.enter(other_second)
        state["attend"] = attend_back(
            items,
            middle,
            grad_second,
            other,
            grad_reduced_low,
            row(second_gain),
            merge_weight,
            mixed,
            head_gains,
            probs,
            heads_low,
            heads_weight,
        )
        grad_first = state["attend"][3]
        chain.leave(grad_first)
        state["other_first"] = swap_core(grad_first)

    def run_heads():
        first, scaled = chain.enter(first_low, scaled_low)
        grad_branch, grad_heads = state["attend"][1:3]
        split = lambda array, at, size: array[:, at : at + size]
        half = grad_branch.shape[1] // 2
        state["grads"] = chain.leave(
            *(mult(first, split(grad_heads, k * width, width), LEFT) for k in range(3)),
            *(mult(scaled, split(grad_branch, k * half, half), LEFT) for k in range(2)),
        )

    def run_stem_back():
        (other,) = chain.enter(state["other_first"])
        grad_middle, grad_first = state["attend"][0], state["attend"][3]
        state["stem"] = stem_back(
            patches,
            hidden,
            grad_first,
            other,
            grad_middle,
            row(first_gain),
            image_weight,
            patch_features,
            row(stem_mean),
            row(stem_inverse),
        )
        chain.leave(state["stem"][0])

    def run_image():
        (stem,) = chain.enter(stem_low)
        grad_embedded = state["stem"][1]
        half = grad_embedded.shape[1] // 2
        state["image"] = chain.leave(
            *(mult(stem, grad_embedded[:, k * half : k * half + half], LEFT) for k in range(2))
        )

    def launch_others():
        stack = lambda *arrays: [array.reshape(-1, slot, array.shape[1]) for array in arrays]
        grads, image = state["grads"], state["image"]
        left = stack(grads[0], grads[1], image[0])
        merge = jnp.concatenate([grads[3], grads[4]], axis=0)
        right = stack(grads[2], merge, image[1])
        part = lambda pieces: lambda side: jnp.concatenate([cut(p, side) for p in pieces])
        others.launch(part(left), part(right))

    def small_step():
        steps = lax.axis_size("dp").bit_length() - 1
        bit = state.setdefault("bit", 0)
        if bit == 0:
            attend_sums, stem_sums = state["attend"][4:], state["stem"][3:]
            heads_total = jnp.sum(attend_sums[3].reshape(heads, HEAD_DIM), axis=1)
            table = attend_sums[5][:, : distance_table.shape[1]]
            state["small"] = (*attend_sums[:3], heads_total, attend_sums[4], table, *stem_sums)
            state["small"] += (grad_expand_bias, grad_reduce_bias)
            (packed,) = chain.enter(pack(state["small"]))
        else:
            packed, moved = chain.enter(state["packed"], state["moved"])
            packed = packed + moved
        (state["packed"],) = chain.leave(packed)
        if bit < steps:
            state["moved"] = exchange(packed, bit)
        state["bit"] = bit + 1

    def swap_reduced():
        (value,) = chain.enter(reduced)
        state["reduced"] = value
        state["other_reduced"] = swap_core(value)

    def run_output():
        (other,) = chain.enter(state["other_reduced"])
        block_output = (middle + (state["reduced"] + other) + reduce_bias).astype(jnp.bfloat16)
        (state["output"],) = chain.leave(block_output)

    def run_patch():
        while state["bit"] <= lax.axis_size("dp").bit_length() - 1:
            small_step()
        state["small"] = unpack(state["packed"], state["small"])
        stem_gain_sum, stem_shift_sum = state["small"][8:10]
        (feature,) = chain.enter(patch_features)
        hat = (feature.astype(jnp.float32) - stem_mean) * stem_inverse
        patch_grad = (
            patch_mask[:, None]
            * stem_inverse
            * stem_gain
            * (state["stem"][2] - stem_shift_sum / count - hat * stem_gain_sum / count)
        )
        (state["patch"],) = chain.leave(patch_grad)

    other_second = swap_core(grad_second)
    blocks = {
        "a": run_attend_back,
        "h": run_heads,
        "b": run_stem_back,
        "i": run_image,
        "s": small_step,
        "w": swap_reduced,
        "o": run_output,
        "p": run_patch,
    }
    starts = {"R": launch_reduces, "E": launch_expands, "H": launch_others}
    for step in SCHEDULE.split():
        if step in starts:
            starts.pop(step)()
        elif step in streams:
            streams[step].step()
        else:
            blocks[step]()
    last = {name: stream.finish() for name, stream in streams.items()}
    grad_reduce_weight = jnp.concatenate([piece(entry, 0, 1) for entry in last["R"]], axis=0)
    grad_expand_weight = jnp.concatenate([piece(entry, 0, 1) for entry in last["E"]], axis=1)
    left, right = last["H"]
    model = layer_input.shape[1]
    chunk, deep, image_deep = model // slot, merge_weight.shape[0], image_weight.shape[0] // slot
    grad_query_weight = piece(left, 0, chunk)
    grad_key_weight = piece(left, chunk, 2 * chunk)
    grad_value_weight = piece(right, 0, chunk)
    merge = piece(right, chunk, 2 * chunk)
    grad_merge_weight = jnp.concatenate([merge[:deep], merge[deep:]], axis=1)
    grad_image_weight = jnp.concatenate(
        [
            piece(left, 2 * chunk, 2 * chunk + image_deep),
            piece(right, 2 * chunk, 2 * chunk + image_deep),
        ],
        axis=1,
    )
    (
        grad_second_gain,
        grad_second_shift,
        grad_merge_bias,
        grad_head_gain,
        heads_sums,
        grad_distance_table,
        grad_first_gain,
        grad_first_shift,
        grad_stem_gain,
        grad_stem_shift,
        grad_expand_bias,
        grad_reduce_bias,
    ) = state["small"]
    block_output, input_grad, patch_grad = state["output"], state["stem"][0], state["patch"]
    return (
        block_output,
        input_grad,
        patch_grad,
        grad_query_weight,
        grad_key_weight,
        grad_value_weight,
        grad_merge_weight,
        heads_sums[0, :width],
        heads_sums[0, 2 * width :],
        grad_merge_bias[0],
        grad_head_gain,
        grad_distance_table,
        grad_first_gain[0],
        grad_first_shift[0],
        grad_second_gain[0],
        grad_second_shift[0],
        grad_expand_weight,
        grad_expand_bias[0],
        grad_reduce_weight,
        grad_reduce_bias[0],
        grad_image_weight,
        grad_stem_gain[0],
        grad_stem_shift[0],
    )


def solution(mesh):
    in_specs = (
        P("dp", None),
        P("dp", "tensor"),
        P("dp"),
        P("dp"),
        P("dp", None),
        P(None, "tensor"),
        P(None, "tensor"),
        P(None, "tensor"),
        P("tensor", None),
        P("tensor"),
        P("tensor"),
        P(),
        P("tensor"),
        P("tensor", None),
        P(),
        P(),
        P(),
        P(),
        P(None, "tensor"),
        P("tensor"),
        P("tensor", None),
        P(),
        P("tensor", None),
        P("tensor"),
        P("tensor"),
    )
    out_specs = (
        P("dp", None),
        P("dp", None),
        P("dp", "tensor"),
        P(None, "tensor"),
        P(None, "tensor"),
        P(None, "tensor"),
        P("tensor", None),
        P("tensor"),
        P("tensor"),
        P(),
        P("tensor"),
        P("tensor", None),
        P(),
        P(),
        P(),
        P(),
        P(None, "tensor"),
        P("tensor"),
        P("tensor", None),
        P(),
        P("tensor", None),
        P("tensor"),
        P("tensor"),
    )
    return jax.shard_map(local, mesh=mesh, in_specs=in_specs, out_specs=out_specs, check_vma=False)
```

```python
from functools import partial

import jax
import jax.numpy as jnp
from jax import lax
from jax.experimental import pallas as pl
from jax.experimental.pallas import tpu as pltpu
from jax.sharding import PartitionSpec as P

HEAD_DIM = 64
PATCH_SMALL = 64
PATCH_LARGE = 225
EPSILON = 1e-05
NEGATIVE = -1e30
SCALE = HEAD_DIM ** (-0.5)
LANES = 128
FULL = ((1,), (0,))
RIGHT = ((1,), (1,))
LEFT = ((0,), (0,))
SCHEDULE = " ".join(
    (
        "R a R E",
        "h b i R",
        "E H R s",
        "E R R w",
        "E H H s",
        "R E H s",
        "R H o s",
        "s E R R",
        "H E H E",
        "H p E H",
        "H",
    )
)


def cost(micros):
    return pl.CostEstimate(
        flops=micros * 10**9, transcendentals=0, bytes_accessed=micros * 3 * 10**6
    )


def mult(left, right, dims=FULL):
    return lax.dot_general(left, right, (dims, ((), ())), preferred_element_type=jnp.float32)


def rows_of(length):
    return pl.BlockSpec((length[0], length[1]), lambda item, *_: (item, 0))


def whole(shape):
    return pl.BlockSpec(shape, lambda item, *_: (0,) * len(shape))


def normed(values):
    centered = values - jnp.mean(values, axis=-1, keepdims=True)
    inverse = lax.rsqrt(jnp.mean(centered * centered, axis=-1, keepdims=True) + EPSILON)
    return centered * inverse, inverse


def before(length, limit):
    slots = lax.broadcasted_iota(jnp.int32, (length, 1), 0)
    return jnp.where(slots < limit, 1.0, 0.0).astype(jnp.float32)


def norm_back(normal, inverse, grad, gain):
    scaled = grad * gain
    first = jnp.mean(scaled, axis=-1, keepdims=True)
    second = jnp.mean(scaled * normal, axis=-1, keepdims=True)
    return (scaled - first - normal * second) * inverse


def row_sum(values):
    return jnp.sum(values, axis=0, keepdims=True)


def start_sums(*refs):
    @pl.when(pl.program_id(0) == 0)
    def _():
        for ref in refs:
            ref[...] = jnp.zeros(ref.shape, ref.dtype)


def bias_kernel(table_ref, out_ref):
    length = out_ref.shape[1]
    for head in range(out_ref.shape[0]):
        rows = jnp.broadcast_to(table_ref[head : head + 1, :], (length, 2 * length))
        turned = pltpu.roll(rows, length + 1, 1, stride=1, stride_axis=0)
        out_ref[head] = turned[:, :length]


def distance_bias(table, length):
    heads = table.shape[0]
    padded = jnp.pad(table, ((0, 0), (0, 2 * length - table.shape[1])))
    return pl.pallas_call(
        bias_kernel,
        out_shape=jax.ShapeDtypeStruct((heads, length, length), jnp.float32),
        cost_estimate=cost(2),
        name="distance_bias",
    )(padded)


def half_of(pair, side):
    lanes = lax.broadcasted_iota(jnp.int32, pair.shape, 1)
    keep = lanes < HEAD_DIM if side == 0 else lanes >= HEAD_DIM
    return jnp.where(keep, pair, jnp.zeros_like(pair))


def join(left, right):
    lanes = lax.broadcasted_iota(jnp.int32, left.shape, 1)
    return jnp.where(lanes < HEAD_DIM, left, right)


def attend_kernel(
    patches_ref,
    valid_ref,
    input_ref,
    own_ref,
    other_ref,
    gain_ref,
    shift_ref,
    heads_weight_ref,
    heads_bias_ref,
    bias_ref,
    head_gain_ref,
    merge_ref,
    hidden_ref,
    first_ref,
    heads_ref,
    probs_ref,
    mixed_ref,
    scaled_ref,
    branch_ref,
):
    item = pl.program_id(0)
    length = input_ref.shape[0]
    width = mixed_ref.shape[1]
    mask = before(length, patches_ref[item])
    hidden = input_ref[...].astype(jnp.float32) + mask * (own_ref[...] + other_ref[...])
    hidden_ref[...] = hidden
    normal, _ = normed(hidden)
    first = (normal * gain_ref[...] + shift_ref[...]).astype(jnp.bfloat16)
    first_ref[...] = first
    heads_ref[...] = (mult(first, heads_weight_ref[...]) + heads_bias_ref[...]).astype(jnp.bfloat16)
    slots = lax.broadcasted_iota(jnp.int32, (length, length), 1)
    valid = slots < valid_ref[item]
    for pair in range(width // LANES):
        at = pair * LANES
        queries = heads_ref[:, at : at + LANES]
        keys = heads_ref[:, width + at : width + at + LANES]
        values = heads_ref[:, 2 * width + at : 2 * width + at + LANES]
        halves = []
        for side in range(2):
            head = 2 * pair + side
            scores = mult(half_of(queries, side), keys, RIGHT) * SCALE + bias_ref[head]
            scores = jnp.where(valid, scores, NEGATIVE)
            peak = jnp.max(scores, axis=-1, keepdims=True)
            powers = jnp.exp(scores - peak)
            probs = powers * (1.0 / jnp.sum(powers, axis=-1, keepdims=True))
            probs_ref[0, head] = probs
            halves.append(mult(probs.astype(jnp.bfloat16), values))
        mixed = join(*halves)
        mixed_ref[:, at : at + LANES] = mixed
        gains = head_gain_ref[:, at : at + LANES]
        scaled_ref[:, at : at + LANES] = (mixed * gains).astype(jnp.bfloat16)
    branch_ref[...] = mult(scaled_ref[...], merge_ref[...])


def attend(
    patches,
    valid,
    layer_input,
    own,
    other,
    gain,
    shift,
    heads_weight,
    heads_bias,
    bias,
    head_gain,
    merge,
):
    items = patches.shape[0]
    rows, model = layer_input.shape
    length = rows // items
    width = merge.shape[0]
    heads = bias.shape[0]
    out = lambda columns, kind: jax.ShapeDtypeStruct((rows, columns), kind)
    return pl.pallas_call(
        attend_kernel,
        grid_spec=pltpu.PrefetchScalarGridSpec(
            num_scalar_prefetch=2,
            grid=(items,),
            in_specs=[
                rows_of((length, model)),
                rows_of((length, model)),
                rows_of((length, model)),
                whole((1, model)),
                whole((1, model)),
                whole(heads_weight.shape),
                whole(heads_bias.shape),
                whole(bias.shape),
                whole(head_gain.shape),
                whole(merge.shape),
            ],
            out_specs=[
                rows_of((length, model)),
                rows_of((length, model)),
                rows_of((length, 3 * width)),
                pl.BlockSpec((1, heads, length, length), lambda item, *_: (item, 0, 0, 0)),
                rows_of((length, width)),
                rows_of((length, width)),
                rows_of((length, model)),
            ],
        ),
        out_shape=[
            out(model, jnp.float32),
            out(model, jnp.bfloat16),
            out(3 * width, jnp.bfloat16),
            jax.ShapeDtypeStruct((items, heads, length, length), jnp.float32),
            out(width, jnp.float32),
            out(width, jnp.bfloat16),
            out(model, jnp.float32),
        ],
        cost_estimate=cost(15),
        name="attend",
    )(
        patches,
        valid,
        layer_input,
        own,
        other,
        gain,
        shift,
        heads_weight,
        heads_bias,
        bias,
        head_gain,
        merge,
    )


def gelu_terms(values):
    power = jnp.exp(values * values * -0.5)
    inverse = 1.0 / (1.0 + jnp.abs(values) * 0.23164189)
    tail = 0.5307027
    for factor in (-0.7265760, 0.7107069, -0.14224836, 0.12741479):
        tail = tail * inverse + factor
    tail = tail * inverse * power
    cumulative = jnp.where(values < 0.0, tail, 1.0 - tail)
    return cumulative, cumulative + values * power * 0.3989422804014327


def feed_kernel(
    valid_ref,
    hidden_ref,
    own_ref,
    other_ref,
    merge_bias_ref,
    gain_ref,
    shift_ref,
    expand_ref,
    expand_bias_ref,
    reduce_ref,
    upstream_ref,
    middle_ref,
    second_ref,
    active_ref,
    grad_expanded_ref,
    reduced_ref,
    grad_second_ref,
    grad_reduced_ref,
    expand_sum_ref,
    reduce_sum_ref,
):
    item = pl.program_id(0)
    length = hidden_ref.shape[0]
    start_sums(expand_sum_ref, reduce_sum_ref)
    middle = hidden_ref[...] + (own_ref[...] + other_ref[...]) + merge_bias_ref[...]
    middle_ref[...] = middle
    normal, _ = normed(middle)
    second = (normal * gain_ref[...] + shift_ref[...]).astype(jnp.bfloat16)
    second_ref[...] = second
    grad_result = upstream_ref[...].astype(jnp.float32) * before(length, valid_ref[item])
    reduce_sum_ref[...] += row_sum(grad_result)
    grad_reduced = grad_result.astype(jnp.bfloat16)
    grad_reduced_ref[...] = grad_reduced
    hidden_units = expand_ref.shape[1]
    part = hidden_units // 3
    reduced = None
    for at in range(0, hidden_units, part):
        span = slice(at, at + part)
        expanded = mult(second, expand_ref[:, span]) + expand_bias_ref[:, span]
        cumulative, slope = gelu_terms(expanded)
        active = (expanded * cumulative).astype(jnp.bfloat16)
        active_ref[:, span] = active
        grad_active = mult(grad_reduced, reduce_ref[span, :], RIGHT)
        grad_expanded = (grad_active * slope).astype(jnp.bfloat16)
        grad_expanded_ref[:, span] = grad_expanded
        expand_sum_ref[:, span] += row_sum(grad_expanded.astype(jnp.float32))
        reduced_part = mult(active, reduce_ref[span, :])
        grad_part = mult(grad_expanded, expand_ref[:, span], RIGHT)
        if reduced is None:
            reduced, grad_second = reduced_part, grad_part
        else:
            reduced, grad_second = reduced + reduced_part, grad_second + grad_part
    reduced_ref[...] = reduced
    grad_second_ref[...] = grad_second


def feed(
    valid,
    hidden,
    own,
    other,
    merge_bias,
    gain,
    shift,
    expand,
    expand_bias,
    reduce_weight,
    upstream,
):
    items = valid.shape[0]
    rows, model = hidden.shape
    length = rows // items
    units = expand.shape[1]
    out = lambda columns, kind: jax.ShapeDtypeStruct((rows, columns), kind)
    model_rows = rows_of((length, model))
    unit_rows = rows_of((length, units))
    return pl.pallas_call(
        feed_kernel,
        grid_spec=pltpu.PrefetchScalarGridSpec(
            num_scalar_prefetch=1,
            grid=(items,),
            in_specs=[
                model_rows,
                model_rows,
                model_rows,
                whole((1, model)),
                whole((1, model)),
                whole((1, model)),
                whole(expand.shape),
                whole(expand_bias.shape),
                whole(reduce_weight.shape),
                model_rows,
            ],
            out_specs=[
                model_rows,
                model_rows,
                unit_rows,
                unit_rows,
                model_rows,
                model_rows,
                model_rows,
                whole((1, units)),
                whole((1, model)),
            ],
        ),
        out_shape=[
            out(model, jnp.float32),
            out(model, jnp.bfloat16),
            out(units, jnp.bfloat16),
            out(units, jnp.bfloat16),
            out(model, jnp.float32),
            out(model, jnp.float32),
            out(model, jnp.bfloat16),
            jax.ShapeDtypeStruct((1, units), jnp.float32),
            jax.ShapeDtypeStruct((1, model), jnp.float32),
        ],
        cost_estimate=cost(23),
        name="feed",
    )(
        valid,
        hidden,
        own,
        other,
        merge_bias,
        gain,
        shift,
        expand,
        expand_bias,
        reduce_weight,
        upstream,
    )


def attend_back_kernel(
    middle_ref,
    own_ref,
    other_ref,
    grad_reduced_ref,
    gain_ref,
    merge_ref,
    mixed_ref,
    head_gain_ref,
    probs_ref,
    heads_ref,
    heads_weight_ref,
    grad_middle_ref,
    grad_branch_ref,
    grad_heads_ref,
    grad_first_ref,
    gain_sum_ref,
    shift_sum_ref,
    merge_sum_ref,
    head_sum_ref,
    heads_sum_ref,
    table_ref,
    total_ref,
):
    item = pl.program_id(0)
    length = middle_ref.shape[0]
    width = mixed_ref.shape[1]
    start_sums(gain_sum_ref, shift_sum_ref, merge_sum_ref, head_sum_ref, heads_sum_ref, total_ref)
    normal, inverse = normed(middle_ref[...])
    grad_second = own_ref[...] + other_ref[...]
    gain_sum_ref[...] += row_sum(grad_second * normal)
    shift_sum_ref[...] += row_sum(grad_second)
    grad_middle = grad_reduced_ref[...].astype(jnp.float32) + norm_back(
        normal, inverse, grad_second, gain_ref[...]
    )
    grad_middle_ref[...] = grad_middle
    merge_sum_ref[...] += row_sum(grad_middle)
    grad_branch = grad_middle.astype(jnp.bfloat16)
    grad_branch_ref[...] = grad_branch
    grad_scaled = mult(grad_branch, merge_ref[...], RIGHT)
    head_sum_ref[...] += row_sum(grad_scaled * mixed_ref[...])
    grad_mixed = (grad_scaled * head_gain_ref[...]).astype(jnp.bfloat16)
    for pair in range(width // LANES):
        at = pair * LANES
        spans = [slice(k * width + at, k * width + at + LANES) for k in range(3)]
        queries, keys, values = (heads_ref[:, span] for span in spans)
        grads = grad_mixed[:, at : at + LANES]
        halves = []
        for side in range(2):
            head = 2 * pair + side
            probs = probs_ref[0, head]
            grad_values = mult(probs.astype(jnp.bfloat16), grads, LEFT)
            grad_probs = mult(half_of(grads, side), values, RIGHT)
            weighted = jnp.sum(probs * grad_probs, axis=-1, keepdims=True)
            grad_scores = (probs * (grad_probs - weighted)).astype(jnp.bfloat16)
            total_ref[head] += grad_scores.astype(jnp.float32)
            grad_queries = mult(grad_scores, keys) * SCALE
            grad_keys = mult(grad_scores, queries, LEFT) * SCALE
            halves.append((grad_queries, grad_keys, grad_values))
        for span, left, right in zip(spans, *halves):
            low = join(left, right).astype(jnp.bfloat16)
            grad_heads_ref[:, span] = low
            heads_sum_ref[:, span] += row_sum(low.astype(jnp.float32))
    grad_first_ref[...] = mult(grad_heads_ref[...], heads_weight_ref[...], RIGHT)

    @pl.when(item == pl.num_programs(0) - 1)
    def _():
        blank = jnp.zeros((length, length), jnp.float32)
        for head in range(total_ref.shape[0]):
            wide = jnp.concatenate([blank, total_ref[head]], axis=1)
            slots = length - 1 - lax.broadcasted_iota(jnp.int32, (length, length), 0)
            swap = jnp.where(lax.broadcasted_iota(jnp.int32, (length, length), 1) == slots, 1.0, 0.0)
            turned = lax.dot_general(
                swap,
                wide,
                (FULL, ((), ())),
                precision=lax.Precision.HIGHEST,
                preferred_element_type=jnp.float32,
            )
            turned = pltpu.roll(turned, length, 1, stride=1, stride_axis=0)
            table_ref[head : head + 1, :] = row_sum(turned)


def attend_back(
    items,
    middle,
    own,
    other,
    grad_reduced,
    gain,
    merge,
    mixed,
    head_gain,
    probs,
    heads_low,
    heads_weight,
):
    rows, model = middle.shape
    length = rows // items
    width = merge.shape[0]
    heads = probs.shape[1]
    out = lambda columns, kind: jax.ShapeDtypeStruct((rows, columns), kind)
    model_rows = rows_of((length, model))
    sums = lambda columns: jax.ShapeDtypeStruct((1, columns), jnp.float32)
    return pl.pallas_call(
        attend_back_kernel,
        grid_spec=pltpu.PrefetchScalarGridSpec(
            num_scalar_prefetch=0,
            grid=(items,),
            in_specs=[
                model_rows,
                model_rows,
                model_rows,
                model_rows,
                whole((1, model)),
                whole(merge.shape),
                rows_of((length, width)),
                whole(head_gain.shape),
                pl.BlockSpec((1, heads, length, length), lambda item, *_: (item, 0, 0, 0)),
                rows_of((length, 3 * width)),
                whole(heads_weight.shape),
            ],
            out_specs=[
                model_rows,
                model_rows,
                rows_of((length, 3 * width)),
                model_rows,
                whole((1, model)),
                whole((1, model)),
                whole((1, model)),
                whole((1, width)),
                whole((1, 3 * width)),
                whole((heads, 2 * length)),
            ],
            scratch_shapes=[pltpu.VMEM((heads, length, length), jnp.float32)],
        ),
        out_shape=[
            out(model, jnp.float32),
            out(model, jnp.bfloat16),
            out(3 * width, jnp.bfloat16),
            out(model, jnp.float32),
            sums(model),
            sums(model),
            sums(model),
            sums(width),
            sums(3 * width),
            jax.ShapeDtypeStruct((heads, 2 * length), jnp.float32),
        ],
        cost_estimate=cost(24),
        name="attend_back",
    )(
        middle,
        own,
        other,
        grad_reduced,
        gain,
        merge,
        mixed,
        head_gain,
        probs,
        heads_low,
        heads_weight,
    )


def stem_back_kernel(
    patches_ref,
    hidden_ref,
    own_ref,
    other_ref,
    grad_middle_ref,
    gain_ref,
    image_ref,
    features_ref,
    mean_ref,
    inverse_ref,
    input_grad_ref,
    grad_embedded_ref,
    grad_stem_ref,
    gain_sum_ref,
    shift_sum_ref,
    stem_gain_ref,
    stem_shift_ref,
):
    item = pl.program_id(0)
    length = hidden_ref.shape[0]
    start_sums(gain_sum_ref, shift_sum_ref, stem_gain_ref, stem_shift_ref)
    normal, inverse = normed(hidden_ref[...])
    grad_first = own_ref[...] + other_ref[...]
    gain_sum_ref[...] += row_sum(grad_first * normal)
    shift_sum_ref[...] += row_sum(grad_first)
    input_grad = grad_middle_ref[...] + norm_back(normal, inverse, grad_first, gain_ref[...])
    input_grad_ref[...] = input_grad
    mask = before(length, patches_ref[item])
    grad_embedded = (input_grad * mask).astype(jnp.bfloat16)
    grad_embedded_ref[...] = grad_embedded
    grad_stem = mult(grad_embedded, image_ref[...], RIGHT)
    grad_stem_ref[...] = grad_stem
    stem_hat = (features_ref[...].astype(jnp.float32) - mean_ref[...]) * inverse_ref[...]
    stem_shift_ref[...] += row_sum(grad_stem)
    stem_gain_ref[...] += row_sum(grad_stem * stem_hat)


def stem_back(
    patches, hidden, own, other, grad_middle, gain, image, features, mean, inverse
):
    items = patches.shape[0]
    rows, model = hidden.shape
    length = rows // items
    channels = features.shape[1]
    out = lambda columns, kind: jax.ShapeDtypeStruct((rows, columns), kind)
    model_rows = rows_of((length, model))
    channel_rows = rows_of((length, channels))
    sums = lambda columns: jax.ShapeDtypeStruct((1, columns), jnp.float32)
    return pl.pallas_call(
        stem_back_kernel,
        grid_spec=pltpu.PrefetchScalarGridSpec(
            num_scalar_prefetch=1,
            grid=(items,),
            in_specs=[
                model_rows,
                model_rows,
                model_rows,
                model_rows,
                whole((1, model)),
                whole(image.shape),
                channel_rows,
                whole((1, channels)),
                whole((1, channels)),
            ],
            out_specs=[
                model_rows,
                model_rows,
                channel_rows,
                whole((1, model)),
                whole((1, model)),
                whole((1, channels)),
                whole((1, channels)),
            ],
        ),
        out_shape=[
            out(model, jnp.float32),
            out(model, jnp.bfloat16),
            out(channels, jnp.float32),
            sums(model),
            sums(model),
            sums(channels),
            sums(channels),
        ],
        cost_estimate=cost(10),
        name="stem_back",
    )(patches, hidden, own, other, grad_middle, gain, image, features, mean, inverse)


def swap_core(values):
    count = lax.axis_size("tensor")
    return lax.ppermute(values, "tensor", [(core, core ^ 1) for core in range(count)])


def exchange(values, bit):
    count = lax.axis_size("dp")
    return lax.ppermute(values, "dp", [(rank, rank ^ (1 << bit)) for rank in range(count)])


def sum_by_doubling(values):
    for bit in range(lax.axis_size("dp").bit_length() - 1):
        values = values + exchange(values, bit)
    return values


class Chain:
    def __init__(self):
        self.token = ()

    def enter(self, *arrays):
        held = lax.optimization_barrier((*self.token, *arrays))
        return held[len(self.token) :]

    def leave(self, *arrays):
        self.token = arrays
        return arrays


def cut(values, side):
    half = values.shape[1] // 2
    return lax.dynamic_slice_in_dim(values, side * half, half, 1)


def spread(side, mine, other):
    return jnp.where(
        side == 1,
        jnp.concatenate([other, mine], axis=1),
        jnp.concatenate([mine, other], axis=1),
    )


def regroup(arrays, count):
    if len(arrays) == count:
        return list(arrays)
    if count == 1:
        return [jnp.concatenate(arrays, axis=0)]
    return list(jnp.split(arrays[0], count, axis=0))


class Stream:
    def __init__(self, chain):
        bits = lax.axis_size("dp").bit_length() - 1
        self.chain = chain
        self.rank = lax.axis_index("dp")
        self.plan = ((0, 1), (1, 0)) + tuple((bit,) for bit in range(2, bits))
        self.stage = 0

    def bits(self, stage):
        steps = self.plan + self.plan[::-1]
        return steps[stage]

    def sides(self, stage):
        return [(self.rank >> bit) & 1 for bit in self.bits(stage)]

    def send(self, arrays):
        arrays = self.chain.leave(*arrays)
        self.flight = [exchange(array, bit) for array, bit in zip(arrays, self.bits(self.stage))]

    def launch(self, *parts):
        sides = self.sides(0)
        self.send([part(1 - side) for part, side in zip(parts, sides)])
        self.kept = [part(side) for part, side in zip(parts, sides)]

    def step(self):
        steps = len(self.plan)
        if self.stage == 2 * steps:
            return
        held = self.chain.enter(*self.flight)
        self.stage += 1
        if self.stage < steps:
            count = len(self.bits(self.stage))
            kept, held = regroup(self.kept, count), regroup(held, count)
            sides = self.sides(self.stage)
            pairs = list(zip(kept, held, sides))
            self.send([cut(mine, 1 - side) + cut(other, 1 - side) for mine, other, side in pairs])
            self.kept = [cut(mine, side) + cut(other, side) for mine, other, side in pairs]
        elif self.stage == steps:
            self.values = [mine + other for mine, other in zip(self.kept, held)]
            self.send(self.values)
        else:
            sides = self.sides(self.stage - 1)
            self.last = list(zip(sides, self.values, held))
            if self.stage < 2 * steps:
                values = [spread(*entry) for entry in self.last]
                self.values = regroup(values, len(self.bits(self.stage)))
                self.send(self.values)
            else:
                self.chain.leave(*held)

    def finish(self):
        while self.stage < 2 * len(self.plan):
            self.step()
        return self.last


def piece(entry, start, stop):
    side, mine, other = entry
    whole_rows = spread(side, mine[start:stop], other[start:stop])
    return whole_rows.reshape(-1, whole_rows.shape[2])


def local(
    layer_input,
    patch_features,
    bucket_ids,
    text_lengths,
    upstream,
    query_weight,
    key_weight,
    value_weight,
    merge_weight,
    query_bias,
    value_bias,
    merge_bias,
    head_gain,
    distance_table,
    first_gain,
    first_shift,
    second_gain,
    second_shift,
    expand_weight,
    expand_bias,
    reduce_weight,
    reduce_bias,
    image_weight,
    stem_gain,
    stem_shift,
):
    items = bucket_ids.shape[0]
    rows = layer_input.shape[0]
    length = rows // items
    heads = head_gain.shape[0]
    width = query_weight.shape[1]
    row = lambda vector: vector.reshape(1, -1)
    patches = PATCH_SMALL + (PATCH_LARGE - PATCH_SMALL) * bucket_ids
    valid = patches + text_lengths
    slots = jnp.arange(length, dtype=jnp.int32)
    patch_mask = (slots[None, :] < patches[:, None]).astype(jnp.float32).reshape(rows)
    features = patch_features.astype(jnp.float32)
    masked = features * patch_mask[:, None]
    feature_sum, square_sum, count = sum_by_doubling(
        jnp.stack(
            [
                jnp.sum(masked, axis=0),
                jnp.sum(masked * features, axis=0),
                jnp.full((features.shape[1],), jnp.sum(patch_mask)),
            ]
        )
    )
    bias = distance_bias(distance_table, length)
    heads_weight = jnp.concatenate([query_weight, key_weight, value_weight], axis=1)
    heads_bias = row(jnp.concatenate([query_bias, jnp.zeros_like(query_bias), value_bias]))
    head_gains = row(jnp.repeat(head_gain, HEAD_DIM))
    stem_mean = feature_sum / count
    stem_inverse = lax.rsqrt(square_sum / count - stem_mean * stem_mean + EPSILON)
    stem_hat = (features - stem_mean) * stem_inverse
    stem_low = (stem_hat * stem_gain + stem_shift).astype(jnp.bfloat16)
    embedded = mult(stem_low, image_weight)
    hidden, first_low, heads_low, probs, mixed, scaled_low, branch = attend(
        patches,
        valid,
        layer_input,
        embedded,
        swap_core(embedded),
        row(first_gain),
        row(first_shift),
        heads_weight,
        heads_bias,
        bias,
        head_gains,
        merge_weight,
    )
    (
        middle,
        second_low,
        active_low,
        grad_expanded_low,
        reduced,
        grad_second,
        grad_reduced_low,
        grad_expand_bias,
        grad_reduce_bias,
    ) = feed(
        valid,
        hidden,
        branch,
        swap_core(branch),
        row(merge_bias),
        row(second_gain),
        row(second_shift),
        expand_weight,
        row(expand_bias),
        reduce_weight,
        upstream,
    )
    chain = Chain()
    reduces, expands, others = Stream(chain), Stream(chain), Stream(chain)
    streams = {"R": reduces, "E": expands, "H": others}
    slot = 256
    state = {}

    def reduce_part(at, size):
        def part(side):
            units = lax.dynamic_slice_in_dim(active_low, at + side * (size // 2), size // 2, 1)
            return mult(units, grad_reduced_low, LEFT)[None]

        return part

    def expand_part(at, size):
        def part(side):
            half = second_low.shape[1] // 2
            columns = lax.dynamic_slice_in_dim(state["second"], side * half, half, 1)
            return mult(columns, grad_expanded_low[:, at : at + size], LEFT)[None]

        return part

    def launch_reduces():
        size = active_low.shape[1] // 2
        reduces.launch(reduce_part(0, size), reduce_part(size, size))

    def launch_expands():
        (state["second"],) = chain.enter(second_low)
        size = grad_expanded_low.shape[1] // 2
        expands.launch(expand_part(0, size), expand_part(size, size))

    def run_attend_back():
        (other,) = chain.enter(other_second)
        state["attend"] = attend_back(
            items,
            middle,
            grad_second,
            other,
            grad_reduced_low,
            row(second_gain),
            merge_weight,
            mixed,
            head_gains,
            probs,
            heads_low,
            heads_weight,
        )
        grad_first = state["attend"][3]
        chain.leave(grad_first)
        state["other_first"] = swap_core(grad_first)

    def run_heads():
        first, scaled = chain.enter(first_low, scaled_low)
        grad_branch, grad_heads = state["attend"][1:3]
        split = lambda array, at, size: array[:, at : at + size]
        half = grad_branch.shape[1] // 2
        state["grads"] = chain.leave(
            *(mult(first, split(grad_heads, k * width, width), LEFT) for k in range(3)),
            *(mult(scaled, split(grad_branch, k * half, half), LEFT) for k in range(2)),
        )

    def run_stem_back():
        (other,) = chain.enter(state["other_first"])
        grad_middle, grad_first = state["attend"][0], state["attend"][3]
        state["stem"] = stem_back(
            patches,
            hidden,
            grad_first,
            other,
            grad_middle,
            row(first_gain),
            image_weight,
            patch_features,
            row(stem_mean),
            row(stem_inverse),
        )
        chain.leave(state["stem"][0])

    def run_image():
        (stem,) = chain.enter(stem_low)
        grad_embedded = state["stem"][1]
        half = grad_embedded.shape[1] // 2
        state["image"] = chain.leave(
            *(mult(stem, grad_embedded[:, k * half : k * half + half], LEFT) for k in range(2))
        )

    def launch_others():
        stack = lambda *arrays: [array.reshape(-1, slot, array.shape[1]) for array in arrays]
        grads, image = state["grads"], state["image"]
        left = stack(grads[0], grads[1], image[0])
        merge = jnp.concatenate([grads[3], grads[4]], axis=0)
        right = stack(grads[2], merge, image[1])
        part = lambda pieces: lambda side: jnp.concatenate([cut(p, side) for p in pieces])
        others.launch(part(left), part(right))

    def small_step():
        steps = lax.axis_size("dp").bit_length() - 1
        bit = state.setdefault("bit", 0)
        if bit == 0:
            attend_sums, stem_sums = state["attend"][4:], state["stem"][3:]
            table = [attend_sums[5][head : head + 1] for head in range(heads)]
            state["small"] = (*attend_sums[:5], *stem_sums, grad_expand_bias, grad_reduce_bias)
            state["small"] += tuple(table)
            (packed,) = chain.enter(jnp.concatenate(state["small"], axis=1))
        else:
            packed, moved = chain.enter(state["packed"], state["moved"])
            packed = packed + moved
        (state["packed"],) = chain.leave(packed)
        if bit < steps:
            state["moved"] = exchange(packed, bit)
        state["bit"] = bit + 1

    def swap_reduced():
        (value,) = chain.enter(reduced)
        state["reduced"] = value
        state["other_reduced"] = swap_core(value)

    def run_output():
        (other,) = chain.enter(state["other_reduced"])
        block_output = (middle + (state["reduced"] + other) + reduce_bias).astype(jnp.bfloat16)
        (state["output"],) = chain.leave(block_output)

    def run_patch():
        while state["bit"] <= lax.axis_size("dp").bit_length() - 1:
            small_step()
        at, parts = 0, []
        for entry in state["small"]:
            parts.append(state["packed"][:, at : at + entry.shape[1]])
            at += entry.shape[1]
        state["small"] = parts
        stem_gain_sum, stem_shift_sum = state["small"][7:9]
        (feature,) = chain.enter(patch_features)
        hat = (feature.astype(jnp.float32) - stem_mean) * stem_inverse
        patch_grad = (
            patch_mask[:, None]
            * stem_inverse
            * stem_gain
            * (state["stem"][2] - stem_shift_sum / count - hat * stem_gain_sum / count)
        )
        (state["patch"],) = chain.leave(patch_grad)

    other_second = swap_core(grad_second)
    blocks = {
        "a": run_attend_back,
        "h": run_heads,
        "b": run_stem_back,
        "i": run_image,
        "s": small_step,
        "w": swap_reduced,
        "o": run_output,
        "p": run_patch,
    }
    starts = {"R": launch_reduces, "E": launch_expands, "H": launch_others}
    for step in SCHEDULE.split():
        if step in starts:
            starts.pop(step)()
        elif step in streams:
            streams[step].step()
        else:
            blocks[step]()
    last = {name: stream.finish() for name, stream in streams.items()}
    grad_reduce_weight = jnp.concatenate([piece(entry, 0, 1) for entry in last["R"]], axis=0)
    grad_expand_weight = jnp.concatenate([piece(entry, 0, 1) for entry in last["E"]], axis=1)
    left, right = last["H"]
    model = layer_input.shape[1]
    chunk, deep, image_deep = model // slot, merge_weight.shape[0], image_weight.shape[0] // slot
    grad_query_weight = piece(left, 0, chunk)
    grad_key_weight = piece(left, chunk, 2 * chunk)
    grad_value_weight = piece(right, 0, chunk)
    merge = piece(right, chunk, 2 * chunk)
    grad_merge_weight = jnp.concatenate([merge[:deep], merge[deep:]], axis=1)
    grad_image_weight = jnp.concatenate(
        [
            piece(left, 2 * chunk, 2 * chunk + image_deep),
            piece(right, 2 * chunk, 2 * chunk + image_deep),
        ],
        axis=1,
    )
    (
        grad_second_gain,
        grad_second_shift,
        grad_merge_bias,
        head_sums,
        heads_sums,
        grad_first_gain,
        grad_first_shift,
        grad_stem_gain,
        grad_stem_shift,
        grad_expand_bias,
        grad_reduce_bias,
        *table,
    ) = state["small"]
    grad_head_gain = jnp.sum(head_sums.reshape(heads, HEAD_DIM), axis=1)
    grad_distance_table = jnp.concatenate(table, axis=0)[:, : distance_table.shape[1]]
    block_output, input_grad, patch_grad = state["output"], state["stem"][0], state["patch"]
    return (
        block_output,
        input_grad,
        patch_grad,
        grad_query_weight,
        grad_key_weight,
        grad_value_weight,
        grad_merge_weight,
        heads_sums[0, :width],
        heads_sums[0, 2 * width :],
        grad_merge_bias[0],
        grad_head_gain,
        grad_distance_table,
        grad_first_gain[0],
        grad_first_shift[0],
        grad_second_gain[0],
        grad_second_shift[0],
        grad_expand_weight,
        grad_expand_bias[0],
        grad_reduce_weight,
        grad_reduce_bias[0],
        grad_image_weight,
        grad_stem_gain[0],
        grad_stem_shift[0],
    )


def solution(mesh):
    in_specs = (
        P("dp", None),
        P("dp", "tensor"),
        P("dp"),
        P("dp"),
        P("dp", None),
        P(None, "tensor"),
        P(None, "tensor"),
        P(None, "tensor"),
        P("tensor", None),
        P("tensor"),
        P("tensor"),
        P(),
        P("tensor"),
        P("tensor", None),
        P(),
        P(),
        P(),
        P(),
        P(None, "tensor"),
        P("tensor"),
        P("tensor", None),
        P(),
        P("tensor", None),
        P("tensor"),
        P("tensor"),
    )
    out_specs = (
        P("dp", None),
        P("dp", None),
        P("dp", "tensor"),
        P(None, "tensor"),
        P(None, "tensor"),
        P(None, "tensor"),
        P("tensor", None),
        P("tensor"),
        P("tensor"),
        P(),
        P("tensor"),
        P("tensor", None),
        P(),
        P(),
        P(),
        P(),
        P(None, "tensor"),
        P("tensor"),
        P("tensor", None),
        P(),
        P("tensor", None),
        P("tensor"),
        P("tensor"),
    )
    return jax.shard_map(local, mesh=mesh, in_specs=in_specs, out_specs=out_specs, check_vma=False)
```

```python
from functools import partial

import jax
import jax.numpy as jnp
from jax import lax
from jax.experimental import pallas as pl
from jax.experimental.pallas import tpu as pltpu
from jax.sharding import PartitionSpec as P

HEAD_DIM = 64
PATCH_SMALL = 64
PATCH_LARGE = 225
EPSILON = 1e-05
NEGATIVE = -1e30
SCALE = HEAD_DIM ** (-0.5)
LANES = 128
FULL = ((1,), (0,))
RIGHT = ((1,), (1,))
LEFT = ((0,), (0,))
PAIRED = (True, True, True)
SCHEDULE = " ".join(
    (
        "R a R E",
        "h R b i",
        "R E R s",
        "E E R H",
        "w H E R",
        "E H H s",
        "R E R H",
        "s E H H",
        "s E s p",
        "H o E H",
    )
)


def cost(micros):
    return pl.CostEstimate(
        flops=micros * 10**9, transcendentals=0, bytes_accessed=micros * 3 * 10**6
    )


def mult(left, right, dims=FULL):
    return lax.dot_general(left, right, (dims, ((), ())), preferred_element_type=jnp.float32)


def rows_of(length):
    return pl.BlockSpec((length[0], length[1]), lambda item, *_: (item, 0))


def whole(shape):
    return pl.BlockSpec(shape, lambda item, *_: (0,) * len(shape))


def normed(values):
    centered = values - jnp.mean(values, axis=-1, keepdims=True)
    inverse = lax.rsqrt(jnp.mean(centered * centered, axis=-1, keepdims=True) + EPSILON)
    return centered * inverse, inverse


def before(length, limit):
    slots = lax.broadcasted_iota(jnp.int32, (length, 1), 0)
    return jnp.where(slots < limit, 1.0, 0.0).astype(jnp.float32)


def norm_back(normal, inverse, grad, gain):
    scaled = grad * gain
    first = jnp.mean(scaled, axis=-1, keepdims=True)
    second = jnp.mean(scaled * normal, axis=-1, keepdims=True)
    return (scaled - first - normal * second) * inverse


def row_sum(values):
    return jnp.sum(values, axis=0, keepdims=True)


def start_sums(*refs):
    @pl.when(pl.program_id(0) == 0)
    def _():
        for ref in refs:
            ref[...] = jnp.zeros(ref.shape, ref.dtype)


def bias_kernel(table_ref, out_ref):
    length = out_ref.shape[1]
    for head in range(out_ref.shape[0]):
        rows = jnp.broadcast_to(table_ref[head : head + 1, :], (length, 2 * length))
        turned = pltpu.roll(rows, length + 1, 1, stride=1, stride_axis=0)
        out_ref[head] = turned[:, :length]


def distance_bias(table, length):
    heads = table.shape[0]
    padded = jnp.pad(table, ((0, 0), (0, 2 * length - table.shape[1])))
    return pl.pallas_call(
        bias_kernel,
        out_shape=jax.ShapeDtypeStruct((heads, length, length), jnp.float32),
        cost_estimate=cost(2),
        name="distance_bias",
    )(padded)


def half_of(pair, side):
    lanes = lax.broadcasted_iota(jnp.int32, pair.shape, 1)
    keep = lanes < HEAD_DIM if side == 0 else lanes >= HEAD_DIM
    return jnp.where(keep, pair, jnp.zeros_like(pair))


def join(left, right):
    lanes = lax.broadcasted_iota(jnp.int32, left.shape, 1)
    return jnp.where(lanes < HEAD_DIM, left, right)


def attend_kernel(
    patches_ref,
    valid_ref,
    input_ref,
    own_ref,
    other_ref,
    gain_ref,
    shift_ref,
    heads_weight_ref,
    heads_bias_ref,
    bias_ref,
    head_gain_ref,
    merge_ref,
    hidden_ref,
    first_ref,
    heads_ref,
    probs_ref,
    mixed_ref,
    scaled_ref,
    branch_ref,
):
    item = pl.program_id(0)
    length = input_ref.shape[0]
    width = mixed_ref.shape[1]
    mask = before(length, patches_ref[item])
    hidden = input_ref[...].astype(jnp.float32) + mask * (own_ref[...] + other_ref[...])
    hidden_ref[...] = hidden
    normal, _ = normed(hidden)
    first = (normal * gain_ref[...] + shift_ref[...]).astype(jnp.bfloat16)
    first_ref[...] = first
    heads_ref[...] = (mult(first, heads_weight_ref[...]) + heads_bias_ref[...]).astype(jnp.bfloat16)
    slots = lax.broadcasted_iota(jnp.int32, (length, length), 1)
    valid = slots < valid_ref[item]
    for pair in range(width // LANES):
        at = pair * LANES
        queries = heads_ref[:, at : at + LANES]
        keys = heads_ref[:, width + at : width + at + LANES]
        values = heads_ref[:, 2 * width + at : 2 * width + at + LANES]
        halves = []
        for side in range(2):
            head = 2 * pair + side
            scores = mult(half_of(queries, side), keys, RIGHT) * SCALE + bias_ref[head]
            scores = jnp.where(valid, scores, NEGATIVE)
            peak = jnp.max(scores, axis=-1, keepdims=True)
            powers = jnp.exp(scores - peak)
            probs = powers * (1.0 / jnp.sum(powers, axis=-1, keepdims=True))
            probs_ref[0, head] = probs
            halves.append(mult(probs.astype(jnp.bfloat16), values))
        mixed = join(*halves)
        mixed_ref[:, at : at + LANES] = mixed
        gains = head_gain_ref[:, at : at + LANES]
        scaled_ref[:, at : at + LANES] = (mixed * gains).astype(jnp.bfloat16)
    branch_ref[...] = mult(scaled_ref[...], merge_ref[...])


def attend(
    patches,
    valid,
    layer_input,
    own,
    other,
    gain,
    shift,
    heads_weight,
    heads_bias,
    bias,
    head_gain,
    merge,
):
    items = patches.shape[0]
    rows, model = layer_input.shape
    length = rows // items
    width = merge.shape[0]
    heads = bias.shape[0]
    out = lambda columns, kind: jax.ShapeDtypeStruct((rows, columns), kind)
    return pl.pallas_call(
        attend_kernel,
        grid_spec=pltpu.PrefetchScalarGridSpec(
            num_scalar_prefetch=2,
            grid=(items,),
            in_specs=[
                rows_of((length, model)),
                rows_of((length, model)),
                rows_of((length, model)),
                whole((1, model)),
                whole((1, model)),
                whole(heads_weight.shape),
                whole(heads_bias.shape),
                whole(bias.shape),
                whole(head_gain.shape),
                whole(merge.shape),
            ],
            out_specs=[
                rows_of((length, model)),
                rows_of((length, model)),
                rows_of((length, 3 * width)),
                pl.BlockSpec((1, heads, length, length), lambda item, *_: (item, 0, 0, 0)),
                rows_of((length, width)),
                rows_of((length, width)),
                rows_of((length, model)),
            ],
        ),
        out_shape=[
            out(model, jnp.float32),
            out(model, jnp.bfloat16),
            out(3 * width, jnp.bfloat16),
            jax.ShapeDtypeStruct((items, heads, length, length), jnp.float32),
            out(width, jnp.float32),
            out(width, jnp.bfloat16),
            out(model, jnp.float32),
        ],
        cost_estimate=cost(15),
        name="attend",
    )(
        patches,
        valid,
        layer_input,
        own,
        other,
        gain,
        shift,
        heads_weight,
        heads_bias,
        bias,
        head_gain,
        merge,
    )


def gelu_terms(values):
    power = jnp.exp(values * values * -0.5)
    inverse = 1.0 / (1.0 + jnp.abs(values) * 0.23164189)
    tail = 0.5307027
    for factor in (-0.7265760, 0.7107069, -0.14224836, 0.12741479):
        tail = tail * inverse + factor
    tail = tail * inverse * power
    cumulative = jnp.where(values < 0.0, tail, 1.0 - tail)
    return cumulative, cumulative + values * power * 0.3989422804014327


def feed_kernel(
    valid_ref,
    hidden_ref,
    own_ref,
    other_ref,
    merge_bias_ref,
    gain_ref,
    shift_ref,
    expand_ref,
    expand_bias_ref,
    reduce_ref,
    upstream_ref,
    middle_ref,
    second_ref,
    active_ref,
    grad_expanded_ref,
    reduced_ref,
    grad_second_ref,
    grad_reduced_ref,
    expand_sum_ref,
    reduce_sum_ref,
):
    item = pl.program_id(0)
    length = hidden_ref.shape[0]
    start_sums(expand_sum_ref, reduce_sum_ref)
    middle = hidden_ref[...] + (own_ref[...] + other_ref[...]) + merge_bias_ref[...]
    middle_ref[...] = middle
    normal, _ = normed(middle)
    second = (normal * gain_ref[...] + shift_ref[...]).astype(jnp.bfloat16)
    second_ref[...] = second
    grad_result = upstream_ref[...].astype(jnp.float32) * before(length, valid_ref[item])
    reduce_sum_ref[...] += row_sum(grad_result)
    grad_reduced = grad_result.astype(jnp.bfloat16)
    grad_reduced_ref[...] = grad_reduced
    hidden_units = expand_ref.shape[1]
    part = hidden_units // 3
    reduced = None
    for at in range(0, hidden_units, part):
        span = slice(at, at + part)
        expanded = mult(second, expand_ref[:, span]) + expand_bias_ref[:, span]
        cumulative, slope = gelu_terms(expanded)
        active = (expanded * cumulative).astype(jnp.bfloat16)
        active_ref[:, span] = active
        grad_active = mult(grad_reduced, reduce_ref[span, :], RIGHT)
        grad_expanded = (grad_active * slope).astype(jnp.bfloat16)
        grad_expanded_ref[:, span] = grad_expanded
        expand_sum_ref[:, span] += row_sum(grad_expanded.astype(jnp.float32))
        reduced_part = mult(active, reduce_ref[span, :])
        grad_part = mult(grad_expanded, expand_ref[:, span], RIGHT)
        if reduced is None:
            reduced, grad_second = reduced_part, grad_part
        else:
            reduced, grad_second = reduced + reduced_part, grad_second + grad_part
    reduced_ref[...] = reduced
    grad_second_ref[...] = grad_second


def feed(
    valid,
    hidden,
    own,
    other,
    merge_bias,
    gain,
    shift,
    expand,
    expand_bias,
    reduce_weight,
    upstream,
):
    items = valid.shape[0]
    rows, model = hidden.shape
    length = rows // items
    units = expand.shape[1]
    out = lambda columns, kind: jax.ShapeDtypeStruct((rows, columns), kind)
    model_rows = rows_of((length, model))
    unit_rows = rows_of((length, units))
    return pl.pallas_call(
        feed_kernel,
        grid_spec=pltpu.PrefetchScalarGridSpec(
            num_scalar_prefetch=1,
            grid=(items,),
            in_specs=[
                model_rows,
                model_rows,
                model_rows,
                whole((1, model)),
                whole((1, model)),
                whole((1, model)),
                whole(expand.shape),
                whole(expand_bias.shape),
                whole(reduce_weight.shape),
                model_rows,
            ],
            out_specs=[
                model_rows,
                model_rows,
                unit_rows,
                unit_rows,
                model_rows,
                model_rows,
                model_rows,
                whole((1, units)),
                whole((1, model)),
            ],
        ),
        out_shape=[
            out(model, jnp.float32),
            out(model, jnp.bfloat16),
            out(units, jnp.bfloat16),
            out(units, jnp.bfloat16),
            out(model, jnp.float32),
            out(model, jnp.float32),
            out(model, jnp.bfloat16),
            jax.ShapeDtypeStruct((1, units), jnp.float32),
            jax.ShapeDtypeStruct((1, model), jnp.float32),
        ],
        cost_estimate=cost(23),
        name="feed",
    )(
        valid,
        hidden,
        own,
        other,
        merge_bias,
        gain,
        shift,
        expand,
        expand_bias,
        reduce_weight,
        upstream,
    )


def attend_back_kernel(
    middle_ref,
    own_ref,
    other_ref,
    grad_reduced_ref,
    gain_ref,
    merge_ref,
    mixed_ref,
    head_gain_ref,
    probs_ref,
    heads_ref,
    heads_weight_ref,
    grad_middle_ref,
    grad_branch_ref,
    grad_heads_ref,
    grad_first_ref,
    gain_sum_ref,
    shift_sum_ref,
    merge_sum_ref,
    head_sum_ref,
    heads_sum_ref,
    table_ref,
    total_ref,
):
    item = pl.program_id(0)
    length = middle_ref.shape[0]
    width = mixed_ref.shape[1]
    start_sums(gain_sum_ref, shift_sum_ref, merge_sum_ref, head_sum_ref, heads_sum_ref, total_ref)
    normal, inverse = normed(middle_ref[...])
    grad_second = own_ref[...] + other_ref[...]
    gain_sum_ref[...] += row_sum(grad_second * normal)
    shift_sum_ref[...] += row_sum(grad_second)
    grad_middle = grad_reduced_ref[...].astype(jnp.float32) + norm_back(
        normal, inverse, grad_second, gain_ref[...]
    )
    grad_middle_ref[...] = grad_middle
    merge_sum_ref[...] += row_sum(grad_middle)
    grad_branch = grad_middle.astype(jnp.bfloat16)
    grad_branch_ref[...] = grad_branch
    grad_scaled = mult(grad_branch, merge_ref[...], RIGHT)
    head_sum_ref[...] += row_sum(grad_scaled * mixed_ref[...])
    grad_mixed = (grad_scaled * head_gain_ref[...]).astype(jnp.bfloat16)
    for pair in range(width // LANES):
        at = pair * LANES
        spans = [slice(k * width + at, k * width + at + LANES) for k in range(3)]
        queries, keys, values = (heads_ref[:, span] for span in spans)
        grads = grad_mixed[:, at : at + LANES]
        halves = []
        for side in range(2):
            head = 2 * pair + side
            probs = probs_ref[0, head]
            grad_values = mult(probs.astype(jnp.bfloat16), grads, LEFT)
            grad_probs = mult(half_of(grads, side), values, RIGHT)
            weighted = jnp.sum(probs * grad_probs, axis=-1, keepdims=True)
            grad_scores = (probs * (grad_probs - weighted)).astype(jnp.bfloat16)
            total_ref[head] += grad_scores.astype(jnp.float32)
            grad_queries = mult(grad_scores, keys) * SCALE
            grad_keys = mult(grad_scores, queries, LEFT) * SCALE
            halves.append((grad_queries, grad_keys, grad_values))
        for span, left, right in zip(spans, *halves):
            low = join(left, right).astype(jnp.bfloat16)
            grad_heads_ref[:, span] = low
            heads_sum_ref[:, span] += row_sum(low.astype(jnp.float32))
    grad_first_ref[...] = mult(grad_heads_ref[...], heads_weight_ref[...], RIGHT)

    @pl.when(item == pl.num_programs(0) - 1)
    def _():
        blank = jnp.zeros((length, length), jnp.float32)
        for head in range(total_ref.shape[0]):
            wide = jnp.concatenate([blank, total_ref[head]], axis=1)
            slots = length - 1 - lax.broadcasted_iota(jnp.int32, (length, length), 0)
            swap = jnp.where(lax.broadcasted_iota(jnp.int32, (length, length), 1) == slots, 1.0, 0.0)
            turned = lax.dot_general(
                swap,
                wide,
                (FULL, ((), ())),
                precision=lax.Precision.HIGHEST,
                preferred_element_type=jnp.float32,
            )
            turned = pltpu.roll(turned, length, 1, stride=1, stride_axis=0)
            table_ref[head : head + 1, :] = row_sum(turned)


def attend_back(
    items,
    middle,
    own,
    other,
    grad_reduced,
    gain,
    merge,
    mixed,
    head_gain,
    probs,
    heads_low,
    heads_weight,
):
    rows, model = middle.shape
    length = rows // items
    width = merge.shape[0]
    heads = probs.shape[1]
    out = lambda columns, kind: jax.ShapeDtypeStruct((rows, columns), kind)
    model_rows = rows_of((length, model))
    sums = lambda columns: jax.ShapeDtypeStruct((1, columns), jnp.float32)
    return pl.pallas_call(
        attend_back_kernel,
        grid_spec=pltpu.PrefetchScalarGridSpec(
            num_scalar_prefetch=0,
            grid=(items,),
            in_specs=[
                model_rows,
                model_rows,
                model_rows,
                model_rows,
                whole((1, model)),
                whole(merge.shape),
                rows_of((length, width)),
                whole(head_gain.shape),
                pl.BlockSpec((1, heads, length, length), lambda item, *_: (item, 0, 0, 0)),
                rows_of((length, 3 * width)),
                whole(heads_weight.shape),
            ],
            out_specs=[
                model_rows,
                model_rows,
                rows_of((length, 3 * width)),
                model_rows,
                whole((1, model)),
                whole((1, model)),
                whole((1, model)),
                whole((1, width)),
                whole((1, 3 * width)),
                whole((heads, 2 * length)),
            ],
            scratch_shapes=[pltpu.VMEM((heads, length, length), jnp.float32)],
        ),
        out_shape=[
            out(model, jnp.float32),
            out(model, jnp.bfloat16),
            out(3 * width, jnp.bfloat16),
            out(model, jnp.float32),
            sums(model),
            sums(model),
            sums(model),
            sums(width),
            sums(3 * width),
            jax.ShapeDtypeStruct((heads, 2 * length), jnp.float32),
        ],
        cost_estimate=cost(24),
        name="attend_back",
    )(
        middle,
        own,
        other,
        grad_reduced,
        gain,
        merge,
        mixed,
        head_gain,
        probs,
        heads_low,
        heads_weight,
    )


def stem_back_kernel(
    patches_ref,
    hidden_ref,
    own_ref,
    other_ref,
    grad_middle_ref,
    gain_ref,
    image_ref,
    features_ref,
    mean_ref,
    inverse_ref,
    input_grad_ref,
    grad_embedded_ref,
    grad_stem_ref,
    gain_sum_ref,
    shift_sum_ref,
    stem_gain_ref,
    stem_shift_ref,
):
    item = pl.program_id(0)
    length = hidden_ref.shape[0]
    start_sums(gain_sum_ref, shift_sum_ref, stem_gain_ref, stem_shift_ref)
    normal, inverse = normed(hidden_ref[...])
    grad_first = own_ref[...] + other_ref[...]
    gain_sum_ref[...] += row_sum(grad_first * normal)
    shift_sum_ref[...] += row_sum(grad_first)
    input_grad = grad_middle_ref[...] + norm_back(normal, inverse, grad_first, gain_ref[...])
    input_grad_ref[...] = input_grad
    mask = before(length, patches_ref[item])
    grad_embedded = (input_grad * mask).astype(jnp.bfloat16)
    grad_embedded_ref[...] = grad_embedded
    grad_stem = mult(grad_embedded, image_ref[...], RIGHT)
    grad_stem_ref[...] = grad_stem
    stem_hat = (features_ref[...].astype(jnp.float32) - mean_ref[...]) * inverse_ref[...]
    stem_shift_ref[...] += row_sum(grad_stem)
    stem_gain_ref[...] += row_sum(grad_stem * stem_hat)


def stem_back(
    patches, hidden, own, other, grad_middle, gain, image, features, mean, inverse
):
    items = patches.shape[0]
    rows, model = hidden.shape
    length = rows // items
    channels = features.shape[1]
    out = lambda columns, kind: jax.ShapeDtypeStruct((rows, columns), kind)
    model_rows = rows_of((length, model))
    channel_rows = rows_of((length, channels))
    sums = lambda columns: jax.ShapeDtypeStruct((1, columns), jnp.float32)
    return pl.pallas_call(
        stem_back_kernel,
        grid_spec=pltpu.PrefetchScalarGridSpec(
            num_scalar_prefetch=1,
            grid=(items,),
            in_specs=[
                model_rows,
                model_rows,
                model_rows,
                model_rows,
                whole((1, model)),
                whole(image.shape),
                channel_rows,
                whole((1, channels)),
                whole((1, channels)),
            ],
            out_specs=[
                model_rows,
                model_rows,
                channel_rows,
                whole((1, model)),
                whole((1, model)),
                whole((1, channels)),
                whole((1, channels)),
            ],
        ),
        out_shape=[
            out(model, jnp.float32),
            out(model, jnp.bfloat16),
            out(channels, jnp.float32),
            sums(model),
            sums(model),
            sums(channels),
            sums(channels),
        ],
        cost_estimate=cost(10),
        name="stem_back",
    )(patches, hidden, own, other, grad_middle, gain, image, features, mean, inverse)


def swap_core(values):
    count = lax.axis_size("tensor")
    return lax.ppermute(values, "tensor", [(core, core ^ 1) for core in range(count)])


def exchange(values, bit):
    count = lax.axis_size("dp")
    return lax.ppermute(values, "dp", [(rank, rank ^ (1 << bit)) for rank in range(count)])


def sum_by_doubling(values):
    for bit in range(lax.axis_size("dp").bit_length() - 1):
        values = values + exchange(values, bit)
    return values


class Chain:
    def __init__(self):
        self.token = ()

    def enter(self, *arrays):
        held = lax.optimization_barrier((*self.token, *arrays))
        return held[len(self.token) :]

    def leave(self, *arrays):
        self.token = arrays
        return arrays


def cut(values, side):
    half = values.shape[1] // 2
    return lax.dynamic_slice_in_dim(values, side * half, half, 1)


def spread(side, mine, other):
    return jnp.where(
        side == 1,
        jnp.concatenate([other, mine], axis=1),
        jnp.concatenate([mine, other], axis=1),
    )


def regroup(arrays, count):
    if len(arrays) == count:
        return list(arrays)
    if count == 1:
        return [jnp.concatenate(arrays, axis=0)]
    return list(jnp.split(arrays[0], count, axis=0))


class Stream:
    def __init__(self, chain, paired):
        bits = lax.axis_size("dp").bit_length() - 1
        self.chain = chain
        self.rank = lax.axis_index("dp")
        far = tuple((bit,) for bit in range(2, bits))
        if paired:
            far = tuple((bit, min(bit ^ 1, bits - 1)) for bit in range(2, bits))
        self.plan = ((0, 1), (1, 0)) + far
        self.stage = 0

    def bits(self, stage):
        steps = self.plan + self.plan[::-1]
        return steps[stage]

    def sides(self, stage):
        return [(self.rank >> bit) & 1 for bit in self.bits(stage)]

    def send(self, arrays):
        arrays = self.chain.leave(*arrays)
        self.flight = [exchange(array, bit) for array, bit in zip(arrays, self.bits(self.stage))]

    def launch(self, *parts):
        sides = self.sides(0)
        self.send([part(1 - side) for part, side in zip(parts, sides)])
        self.kept = [part(side) for part, side in zip(parts, sides)]

    def step(self):
        steps = len(self.plan)
        if self.stage == 2 * steps:
            return
        held = self.chain.enter(*self.flight)
        self.stage += 1
        if self.stage < steps:
            count = len(self.bits(self.stage))
            kept, held = regroup(self.kept, count), regroup(held, count)
            sides = self.sides(self.stage)
            pairs = list(zip(kept, held, sides))
            self.send([cut(mine, 1 - side) + cut(other, 1 - side) for mine, other, side in pairs])
            self.kept = [cut(mine, side) + cut(other, side) for mine, other, side in pairs]
        elif self.stage == steps:
            self.values = [mine + other for mine, other in zip(self.kept, held)]
            self.send(self.values)
        else:
            sides = self.sides(self.stage - 1)
            self.last = list(zip(sides, self.values, held))
            if self.stage < 2 * steps:
                values = [spread(*entry) for entry in self.last]
                self.values = regroup(values, len(self.bits(self.stage)))
                self.send(self.values)
            else:
                self.chain.leave(*held)

    def finish(self):
        while self.stage < 2 * len(self.plan):
            self.step()
        return self.last


def piece(entry, start, stop):
    side, mine, other = entry
    whole_rows = spread(side, mine[start:stop], other[start:stop])
    return whole_rows.reshape(-1, whole_rows.shape[2])


def local(
    layer_input,
    patch_features,
    bucket_ids,
    text_lengths,
    upstream,
    query_weight,
    key_weight,
    value_weight,
    merge_weight,
    query_bias,
    value_bias,
    merge_bias,
    head_gain,
    distance_table,
    first_gain,
    first_shift,
    second_gain,
    second_shift,
    expand_weight,
    expand_bias,
    reduce_weight,
    reduce_bias,
    image_weight,
    stem_gain,
    stem_shift,
):
    items = bucket_ids.shape[0]
    rows = layer_input.shape[0]
    length = rows // items
    heads = head_gain.shape[0]
    width = query_weight.shape[1]
    row = lambda vector: vector.reshape(1, -1)
    patches = PATCH_SMALL + (PATCH_LARGE - PATCH_SMALL) * bucket_ids
    valid = patches + text_lengths
    slots = jnp.arange(length, dtype=jnp.int32)
    patch_mask = (slots[None, :] < patches[:, None]).astype(jnp.float32).reshape(rows)
    features = patch_features.astype(jnp.float32)
    masked = features * patch_mask[:, None]
    feature_sum, square_sum, count = sum_by_doubling(
        jnp.stack(
            [
                jnp.sum(masked, axis=0),
                jnp.sum(masked * features, axis=0),
                jnp.full((features.shape[1],), jnp.sum(patch_mask)),
            ]
        )
    )
    bias = distance_bias(distance_table, length)
    heads_weight = jnp.concatenate([query_weight, key_weight, value_weight], axis=1)
    heads_bias = row(jnp.concatenate([query_bias, jnp.zeros_like(query_bias), value_bias]))
    head_gains = row(jnp.repeat(head_gain, HEAD_DIM))
    stem_mean = feature_sum / count
    stem_inverse = lax.rsqrt(square_sum / count - stem_mean * stem_mean + EPSILON)
    stem_hat = (features - stem_mean) * stem_inverse
    stem_low = (stem_hat * stem_gain + stem_shift).astype(jnp.bfloat16)
    embedded = mult(stem_low, image_weight)
    hidden, first_low, heads_low, probs, mixed, scaled_low, branch = attend(
        patches,
        valid,
        layer_input,
        embedded,
        swap_core(embedded),
        row(first_gain),
        row(first_shift),
        heads_weight,
        heads_bias,
        bias,
        head_gains,
        merge_weight,
    )
    (
        middle,
        second_low,
        active_low,
        grad_expanded_low,
        reduced,
        grad_second,
        grad_reduced_low,
        grad_expand_bias,
        grad_reduce_bias,
    ) = feed(
        valid,
        hidden,
        branch,
        swap_core(branch),
        row(merge_bias),
        row(second_gain),
        row(second_shift),
        expand_weight,
        row(expand_bias),
        reduce_weight,
        upstream,
    )
    chain = Chain()
    reduces, expands, others = (Stream(chain, paired) for paired in PAIRED)
    streams = {"R": reduces, "E": expands, "H": others}
    slot = 256
    state = {}

    def reduce_part(at, size):
        def part(side):
            units = lax.dynamic_slice_in_dim(active_low, at + side * (size // 2), size // 2, 1)
            return mult(units, grad_reduced_low, LEFT)[None]

        return part

    def expand_part(at, size):
        def part(side):
            half = second_low.shape[1] // 2
            columns = lax.dynamic_slice_in_dim(state["second"], side * half, half, 1)
            return mult(columns, grad_expanded_low[:, at : at + size], LEFT)[None]

        return part

    def launch_reduces():
        size = active_low.shape[1] // 2
        reduces.launch(reduce_part(0, size), reduce_part(size, size))

    def launch_expands():
        (state["second"],) = chain.enter(second_low)
        size = grad_expanded_low.shape[1] // 2
        expands.launch(expand_part(0, size), expand_part(size, size))

    def run_attend_back():
        (other,) = chain.enter(other_second)
        state["attend"] = attend_back(
            items,
            middle,
            grad_second,
            other,
            grad_reduced_low,
            row(second_gain),
            merge_weight,
            mixed,
            head_gains,
            probs,
            heads_low,
            heads_weight,
        )
        grad_first = state["attend"][3]
        chain.leave(grad_first)
        state["other_first"] = swap_core(grad_first)

    def run_heads():
        first, scaled = chain.enter(first_low, scaled_low)
        grad_branch, grad_heads = state["attend"][1:3]
        split = lambda array, at, size: array[:, at : at + size]
        half = grad_branch.shape[1] // 2
        state["grads"] = chain.leave(
            *(mult(first, split(grad_heads, k * width, width), LEFT) for k in range(3)),
            *(mult(scaled, split(grad_branch, k * half, half), LEFT) for k in range(2)),
        )

    def run_stem_back():
        (other,) = chain.enter(state["other_first"])
        grad_middle, grad_first = state["attend"][0], state["attend"][3]
        state["stem"] = stem_back(
            patches,
            hidden,
            grad_first,
            other,
            grad_middle,
            row(first_gain),
            image_weight,
            patch_features,
            row(stem_mean),
            row(stem_inverse),
        )
        chain.leave(state["stem"][0])

    def run_image():
        (stem,) = chain.enter(stem_low)
        grad_embedded = state["stem"][1]
        half = grad_embedded.shape[1] // 2
        state["image"] = chain.leave(
            *(mult(stem, grad_embedded[:, k * half : k * half + half], LEFT) for k in range(2))
        )

    def launch_others():
        stack = lambda *arrays: [array.reshape(-1, slot, array.shape[1]) for array in arrays]
        grads, image = state["grads"], state["image"]
        left = stack(grads[0], grads[1], image[0])
        merge = jnp.concatenate([grads[3], grads[4]], axis=0)
        right = stack(grads[2], merge, image[1])
        part = lambda pieces: lambda side: jnp.concatenate([cut(p, side) for p in pieces])
        others.launch(part(left), part(right))

    def small_step():
        steps = lax.axis_size("dp").bit_length() - 1
        bit = state.setdefault("bit", 0)
        if bit == 0:
            attend_sums, stem_sums = state["attend"][4:], state["stem"][3:]
            table = [attend_sums[5][head : head + 1] for head in range(heads)]
            state["small"] = (*attend_sums[:5], *stem_sums, grad_expand_bias, grad_reduce_bias)
            state["small"] += tuple(table)
            (packed,) = chain.enter(jnp.concatenate(state["small"], axis=1))
        else:
            packed, moved = chain.enter(state["packed"], state["moved"])
            packed = packed + moved
        (state["packed"],) = chain.leave(packed)
        if bit < steps:
            state["moved"] = exchange(packed, bit)
        state["bit"] = bit + 1

    def swap_reduced():
        (value,) = chain.enter(reduced)
        state["reduced"] = value
        state["other_reduced"] = swap_core(value)

    def run_output():
        (other,) = chain.enter(state["other_reduced"])
        block_output = (middle + (state["reduced"] + other) + reduce_bias).astype(jnp.bfloat16)
        (state["output"],) = chain.leave(block_output)

    def run_patch():
        while state["bit"] <= lax.axis_size("dp").bit_length() - 1:
            small_step()
        at, parts = 0, []
        for entry in state["small"]:
            parts.append(state["packed"][:, at : at + entry.shape[1]])
            at += entry.shape[1]
        state["small"] = parts
        stem_gain_sum, stem_shift_sum = state["small"][7:9]
        (feature,) = chain.enter(patch_features)
        hat = (feature.astype(jnp.float32) - stem_mean) * stem_inverse
        patch_grad = (
            patch_mask[:, None]
            * stem_inverse
            * stem_gain
            * (state["stem"][2] - stem_shift_sum / count - hat * stem_gain_sum / count)
        )
        (state["patch"],) = chain.leave(patch_grad)

    other_second = swap_core(grad_second)
    blocks = {
        "a": run_attend_back,
        "h": run_heads,
        "b": run_stem_back,
        "i": run_image,
        "s": small_step,
        "w": swap_reduced,
        "o": run_output,
        "p": run_patch,
    }
    starts = {"R": launch_reduces, "E": launch_expands, "H": launch_others}
    for step in SCHEDULE.split():
        if step in starts:
            starts.pop(step)()
        elif step in streams:
            streams[step].step()
        else:
            blocks[step]()
    last = {name: stream.finish() for name, stream in streams.items()}
    grad_reduce_weight = jnp.concatenate([piece(entry, 0, 1) for entry in last["R"]], axis=0)
    grad_expand_weight = jnp.concatenate([piece(entry, 0, 1) for entry in last["E"]], axis=1)
    left, right = last["H"]
    model = layer_input.shape[1]
    chunk, deep, image_deep = model // slot, merge_weight.shape[0], image_weight.shape[0] // slot
    grad_query_weight = piece(left, 0, chunk)
    grad_key_weight = piece(left, chunk, 2 * chunk)
    grad_value_weight = piece(right, 0, chunk)
    merge = piece(right, chunk, 2 * chunk)
    grad_merge_weight = jnp.concatenate([merge[:deep], merge[deep:]], axis=1)
    grad_image_weight = jnp.concatenate(
        [
            piece(left, 2 * chunk, 2 * chunk + image_deep),
            piece(right, 2 * chunk, 2 * chunk + image_deep),
        ],
        axis=1,
    )
    (
        grad_second_gain,
        grad_second_shift,
        grad_merge_bias,
        head_sums,
        heads_sums,
        grad_first_gain,
        grad_first_shift,
        grad_stem_gain,
        grad_stem_shift,
        grad_expand_bias,
        grad_reduce_bias,
        *table,
    ) = state["small"]
    grad_head_gain = jnp.sum(head_sums.reshape(heads, HEAD_DIM), axis=1)
    grad_distance_table = jnp.concatenate(table, axis=0)[:, : distance_table.shape[1]]
    block_output, input_grad, patch_grad = state["output"], state["stem"][0], state["patch"]
    return (
        block_output,
        input_grad,
        patch_grad,
        grad_query_weight,
        grad_key_weight,
        grad_value_weight,
        grad_merge_weight,
        heads_sums[0, :width],
        heads_sums[0, 2 * width :],
        grad_merge_bias[0],
        grad_head_gain,
        grad_distance_table,
        grad_first_gain[0],
        grad_first_shift[0],
        grad_second_gain[0],
        grad_second_shift[0],
        grad_expand_weight,
        grad_expand_bias[0],
        grad_reduce_weight,
        grad_reduce_bias[0],
        grad_image_weight,
        grad_stem_gain[0],
        grad_stem_shift[0],
    )


def solution(mesh):
    in_specs = (
        P("dp", None),
        P("dp", "tensor"),
        P("dp"),
        P("dp"),
        P("dp", None),
        P(None, "tensor"),
        P(None, "tensor"),
        P(None, "tensor"),
        P("tensor", None),
        P("tensor"),
        P("tensor"),
        P(),
        P("tensor"),
        P("tensor", None),
        P(),
        P(),
        P(),
        P(),
        P(None, "tensor"),
        P("tensor"),
        P("tensor", None),
        P(),
        P("tensor", None),
        P("tensor"),
        P("tensor"),
    )
    out_specs = (
        P("dp", None),
        P("dp", None),
        P("dp", "tensor"),
        P(None, "tensor"),
        P(None, "tensor"),
        P(None, "tensor"),
        P("tensor", None),
        P("tensor"),
        P("tensor"),
        P(),
        P("tensor"),
        P("tensor", None),
        P(),
        P(),
        P(),
        P(),
        P(None, "tensor"),
        P("tensor"),
        P("tensor", None),
        P(),
        P("tensor", None),
        P("tensor"),
        P("tensor"),
    )
    return jax.shard_map(local, mesh=mesh, in_specs=in_specs, out_specs=out_specs, check_vma=False)
```

```python
from functools import partial

import jax
import jax.numpy as jnp
from jax import lax
from jax.experimental import pallas as pl
from jax.experimental.pallas import tpu as pltpu
from jax.sharding import PartitionSpec as P

HEAD_DIM = 64
PATCH_SMALL = 64
PATCH_LARGE = 225
EPSILON = 1e-05
NEGATIVE = -1e30
SCALE = HEAD_DIM ** (-0.5)
LANES = 128
FULL = ((1,), (0,))
RIGHT = ((1,), (1,))
LEFT = ((0,), (0,))
PAIRED = (True, True, True)
SCHEDULE = " ".join(
    (
        "R a R E",
        "h R b i",
        "E R E R",
        "s E R H",
        "w H R E",
        "H H s R",
        "E s E R",
        "H s E H",
        "H s E p",
        "H o E H",
    )
)


def cost(micros):
    return pl.CostEstimate(
        flops=micros * 10**9, transcendentals=0, bytes_accessed=micros * 3 * 10**6
    )


def mult(left, right, dims=FULL):
    return lax.dot_general(left, right, (dims, ((), ())), preferred_element_type=jnp.float32)


def rows_of(length):
    return pl.BlockSpec((length[0], length[1]), lambda item, *_: (item, 0))


def whole(shape):
    return pl.BlockSpec(shape, lambda item, *_: (0,) * len(shape))


def normed(values):
    centered = values - jnp.mean(values, axis=-1, keepdims=True)
    inverse = lax.rsqrt(jnp.mean(centered * centered, axis=-1, keepdims=True) + EPSILON)
    return centered * inverse, inverse


def before(length, limit):
    slots = lax.broadcasted_iota(jnp.int32, (length, 1), 0)
    return jnp.where(slots < limit, 1.0, 0.0).astype(jnp.float32)


def norm_back(normal, inverse, grad, gain):
    scaled = grad * gain
    first = jnp.mean(scaled, axis=-1, keepdims=True)
    second = jnp.mean(scaled * normal, axis=-1, keepdims=True)
    return (scaled - first - normal * second) * inverse


def row_sum(values):
    return jnp.sum(values, axis=0, keepdims=True)


def start_sums(*refs):
    @pl.when(pl.program_id(0) == 0)
    def _():
        for ref in refs:
            ref[...] = jnp.zeros(ref.shape, ref.dtype)


def bias_kernel(table_ref, out_ref):
    length = out_ref.shape[1]
    for head in range(out_ref.shape[0]):
        rows = jnp.broadcast_to(table_ref[head : head + 1, :], (length, 2 * length))
        turned = pltpu.roll(rows, length + 1, 1, stride=1, stride_axis=0)
        out_ref[head] = turned[:, :length]


def distance_bias(table, length):
    heads = table.shape[0]
    padded = jnp.pad(table, ((0, 0), (0, 2 * length - table.shape[1])))
    return pl.pallas_call(
        bias_kernel,
        out_shape=jax.ShapeDtypeStruct((heads, length, length), jnp.float32),
        cost_estimate=cost(2),
        name="distance_bias",
    )(padded)


def half_of(pair, side):
    lanes = lax.broadcasted_iota(jnp.int32, pair.shape, 1)
    keep = lanes < HEAD_DIM if side == 0 else lanes >= HEAD_DIM
    return jnp.where(keep, pair, jnp.zeros_like(pair))


def join(left, right):
    lanes = lax.broadcasted_iota(jnp.int32, left.shape, 1)
    return jnp.where(lanes < HEAD_DIM, left, right)


def attend_kernel(
    patches_ref,
    valid_ref,
    input_ref,
    own_ref,
    other_ref,
    gain_ref,
    shift_ref,
    heads_weight_ref,
    heads_bias_ref,
    bias_ref,
    head_gain_ref,
    merge_ref,
    hidden_ref,
    first_ref,
    heads_ref,
    probs_ref,
    mixed_ref,
    scaled_ref,
    branch_ref,
):
    item = pl.program_id(0)
    length = input_ref.shape[0]
    width = mixed_ref.shape[1]
    mask = before(length, patches_ref[item])
    hidden = input_ref[...].astype(jnp.float32) + mask * (own_ref[...] + other_ref[...])
    hidden_ref[...] = hidden
    normal, _ = normed(hidden)
    first = (normal * gain_ref[...] + shift_ref[...]).astype(jnp.bfloat16)
    first_ref[...] = first
    heads_ref[...] = (mult(first, heads_weight_ref[...]) + heads_bias_ref[...]).astype(jnp.bfloat16)
    slots = lax.broadcasted_iota(jnp.int32, (length, length), 1)
    valid = slots < valid_ref[item]
    for pair in range(width // LANES):
        at = pair * LANES
        queries = heads_ref[:, at : at + LANES]
        keys = heads_ref[:, width + at : width + at + LANES]
        values = heads_ref[:, 2 * width + at : 2 * width + at + LANES]
        halves = []
        for side in range(2):
            head = 2 * pair + side
            scores = mult(half_of(queries, side), keys, RIGHT) * SCALE + bias_ref[head]
            scores = jnp.where(valid, scores, NEGATIVE)
            peak = jnp.max(scores, axis=-1, keepdims=True)
            powers = jnp.exp(scores - peak)
            probs = powers * (1.0 / jnp.sum(powers, axis=-1, keepdims=True))
            probs_ref[0, head] = probs
            halves.append(mult(probs.astype(jnp.bfloat16), values))
        mixed = join(*halves)
        mixed_ref[:, at : at + LANES] = mixed
        gains = head_gain_ref[:, at : at + LANES]
        scaled_ref[:, at : at + LANES] = (mixed * gains).astype(jnp.bfloat16)
    branch_ref[...] = mult(scaled_ref[...], merge_ref[...])


def attend(
    patches,
    valid,
    layer_input,
    own,
    other,
    gain,
    shift,
    heads_weight,
    heads_bias,
    bias,
    head_gain,
    merge,
):
    items = patches.shape[0]
    rows, model = layer_input.shape
    length = rows // items
    width = merge.shape[0]
    heads = bias.shape[0]
    out = lambda columns, kind: jax.ShapeDtypeStruct((rows, columns), kind)
    return pl.pallas_call(
        attend_kernel,
        grid_spec=pltpu.PrefetchScalarGridSpec(
            num_scalar_prefetch=2,
            grid=(items,),
            in_specs=[
                rows_of((length, model)),
                rows_of((length, model)),
                rows_of((length, model)),
                whole((1, model)),
                whole((1, model)),
                whole(heads_weight.shape),
                whole(heads_bias.shape),
                whole(bias.shape),
                whole(head_gain.shape),
                whole(merge.shape),
            ],
            out_specs=[
                rows_of((length, model)),
                rows_of((length, model)),
                rows_of((length, 3 * width)),
                pl.BlockSpec((1, heads, length, length), lambda item, *_: (item, 0, 0, 0)),
                rows_of((length, width)),
                rows_of((length, width)),
                rows_of((length, model)),
            ],
        ),
        out_shape=[
            out(model, jnp.float32),
            out(model, jnp.bfloat16),
            out(3 * width, jnp.bfloat16),
            jax.ShapeDtypeStruct((items, heads, length, length), jnp.float32),
            out(width, jnp.float32),
            out(width, jnp.bfloat16),
            out(model, jnp.float32),
        ],
        cost_estimate=cost(15),
        name="attend",
    )(
        patches,
        valid,
        layer_input,
        own,
        other,
        gain,
        shift,
        heads_weight,
        heads_bias,
        bias,
        head_gain,
        merge,
    )


def gelu_terms(values):
    power = jnp.exp(values * values * -0.5)
    inverse = 1.0 / (1.0 + jnp.abs(values) * 0.23164189)
    tail = 0.5307027
    for factor in (-0.7265760, 0.7107069, -0.14224836, 0.12741479):
        tail = tail * inverse + factor
    tail = tail * inverse * power
    cumulative = jnp.where(values < 0.0, tail, 1.0 - tail)
    return cumulative, cumulative + values * power * 0.3989422804014327


def feed_kernel(
    valid_ref,
    hidden_ref,
    own_ref,
    other_ref,
    merge_bias_ref,
    gain_ref,
    shift_ref,
    expand_ref,
    expand_bias_ref,
    reduce_ref,
    upstream_ref,
    middle_ref,
    second_ref,
    active_ref,
    grad_expanded_ref,
    reduced_ref,
    grad_second_ref,
    grad_reduced_ref,
    expand_sum_ref,
    reduce_sum_ref,
):
    item = pl.program_id(0)
    length = hidden_ref.shape[0]
    start_sums(expand_sum_ref, reduce_sum_ref)
    middle = hidden_ref[...] + (own_ref[...] + other_ref[...]) + merge_bias_ref[...]
    middle_ref[...] = middle
    normal, _ = normed(middle)
    second = (normal * gain_ref[...] + shift_ref[...]).astype(jnp.bfloat16)
    second_ref[...] = second
    grad_result = upstream_ref[...].astype(jnp.float32) * before(length, valid_ref[item])
    reduce_sum_ref[...] += row_sum(grad_result)
    grad_reduced = grad_result.astype(jnp.bfloat16)
    grad_reduced_ref[...] = grad_reduced
    hidden_units = expand_ref.shape[1]
    part = hidden_units // 3
    reduced = None
    for at in range(0, hidden_units, part):
        span = slice(at, at + part)
        expanded = mult(second, expand_ref[:, span]) + expand_bias_ref[:, span]
        cumulative, slope = gelu_terms(expanded)
        active = (expanded * cumulative).astype(jnp.bfloat16)
        active_ref[:, span] = active
        grad_active = mult(grad_reduced, reduce_ref[span, :], RIGHT)
        grad_expanded = (grad_active * slope).astype(jnp.bfloat16)
        grad_expanded_ref[:, span] = grad_expanded
        expand_sum_ref[:, span] += row_sum(grad_expanded.astype(jnp.float32))
        reduced_part = mult(active, reduce_ref[span, :])
        grad_part = mult(grad_expanded, expand_ref[:, span], RIGHT)
        if reduced is None:
            reduced, grad_second = reduced_part, grad_part
        else:
            reduced, grad_second = reduced + reduced_part, grad_second + grad_part
    reduced_ref[...] = reduced
    grad_second_ref[...] = grad_second


def feed(
    valid,
    hidden,
    own,
    other,
    merge_bias,
    gain,
    shift,
    expand,
    expand_bias,
    reduce_weight,
    upstream,
):
    items = valid.shape[0]
    rows, model = hidden.shape
    length = rows // items
    units = expand.shape[1]
    out = lambda columns, kind: jax.ShapeDtypeStruct((rows, columns), kind)
    model_rows = rows_of((length, model))
    unit_rows = rows_of((length, units))
    return pl.pallas_call(
        feed_kernel,
        grid_spec=pltpu.PrefetchScalarGridSpec(
            num_scalar_prefetch=1,
            grid=(items,),
            in_specs=[
                model_rows,
                model_rows,
                model_rows,
                whole((1, model)),
                whole((1, model)),
                whole((1, model)),
                whole(expand.shape),
                whole(expand_bias.shape),
                whole(reduce_weight.shape),
                model_rows,
            ],
            out_specs=[
                model_rows,
                model_rows,
                unit_rows,
                unit_rows,
                model_rows,
                model_rows,
                model_rows,
                whole((1, units)),
                whole((1, model)),
            ],
        ),
        out_shape=[
            out(model, jnp.float32),
            out(model, jnp.bfloat16),
            out(units, jnp.bfloat16),
            out(units, jnp.bfloat16),
            out(model, jnp.float32),
            out(model, jnp.float32),
            out(model, jnp.bfloat16),
            jax.ShapeDtypeStruct((1, units), jnp.float32),
            jax.ShapeDtypeStruct((1, model), jnp.float32),
        ],
        cost_estimate=cost(23),
        name="feed",
    )(
        valid,
        hidden,
        own,
        other,
        merge_bias,
        gain,
        shift,
        expand,
        expand_bias,
        reduce_weight,
        upstream,
    )


def attend_back_kernel(
    middle_ref,
    own_ref,
    other_ref,
    grad_reduced_ref,
    gain_ref,
    merge_ref,
    mixed_ref,
    head_gain_ref,
    probs_ref,
    heads_ref,
    heads_weight_ref,
    grad_middle_ref,
    grad_branch_ref,
    grad_heads_ref,
    grad_first_ref,
    gain_sum_ref,
    shift_sum_ref,
    merge_sum_ref,
    head_sum_ref,
    heads_sum_ref,
    table_ref,
    total_ref,
):
    item = pl.program_id(0)
    length = middle_ref.shape[0]
    width = mixed_ref.shape[1]
    start_sums(gain_sum_ref, shift_sum_ref, merge_sum_ref, head_sum_ref, heads_sum_ref, total_ref)
    normal, inverse = normed(middle_ref[...])
    grad_second = own_ref[...] + other_ref[...]
    gain_sum_ref[...] += row_sum(grad_second * normal)
    shift_sum_ref[...] += row_sum(grad_second)
    grad_middle = grad_reduced_ref[...].astype(jnp.float32) + norm_back(
        normal, inverse, grad_second, gain_ref[...]
    )
    grad_middle_ref[...] = grad_middle
    merge_sum_ref[...] += row_sum(grad_middle)
    grad_branch = grad_middle.astype(jnp.bfloat16)
    grad_branch_ref[...] = grad_branch
    grad_scaled = mult(grad_branch, merge_ref[...], RIGHT)
    head_sum_ref[...] += row_sum(grad_scaled * mixed_ref[...])
    grad_mixed = (grad_scaled * head_gain_ref[...]).astype(jnp.bfloat16)
    for pair in range(width // LANES):
        at = pair * LANES
        spans = [slice(k * width + at, k * width + at + LANES) for k in range(3)]
        queries, keys, values = (heads_ref[:, span] for span in spans)
        grads = grad_mixed[:, at : at + LANES]
        halves = []
        for side in range(2):
            head = 2 * pair + side
            probs = probs_ref[0, head]
            grad_values = mult(probs.astype(jnp.bfloat16), grads, LEFT)
            grad_probs = mult(half_of(grads, side), values, RIGHT)
            weighted = jnp.sum(probs * grad_probs, axis=-1, keepdims=True)
            grad_scores = (probs * (grad_probs - weighted)).astype(jnp.bfloat16)
            total_ref[head] += grad_scores.astype(jnp.float32)
            grad_queries = mult(grad_scores, keys) * SCALE
            grad_keys = mult(grad_scores, queries, LEFT) * SCALE
            halves.append((grad_queries, grad_keys, grad_values))
        for span, left, right in zip(spans, *halves):
            low = join(left, right).astype(jnp.bfloat16)
            grad_heads_ref[:, span] = low
            heads_sum_ref[:, span] += row_sum(low.astype(jnp.float32))
    grad_first_ref[...] = mult(grad_heads_ref[...], heads_weight_ref[...], RIGHT)

    @pl.when(item == pl.num_programs(0) - 1)
    def _():
        blank = jnp.zeros((length, length), jnp.float32)
        for head in range(total_ref.shape[0]):
            wide = jnp.concatenate([blank, total_ref[head]], axis=1)
            slots = length - 1 - lax.broadcasted_iota(jnp.int32, (length, length), 0)
            swap = jnp.where(lax.broadcasted_iota(jnp.int32, (length, length), 1) == slots, 1.0, 0.0)
            turned = lax.dot_general(
                swap,
                wide,
                (FULL, ((), ())),
                precision=lax.Precision.HIGHEST,
                preferred_element_type=jnp.float32,
            )
            turned = pltpu.roll(turned, length, 1, stride=1, stride_axis=0)
            table_ref[head : head + 1, :] = row_sum(turned)


def attend_back(
    items,
    middle,
    own,
    other,
    grad_reduced,
    gain,
    merge,
    mixed,
    head_gain,
    probs,
    heads_low,
    heads_weight,
):
    rows, model = middle.shape
    length = rows // items
    width = merge.shape[0]
    heads = probs.shape[1]
    out = lambda columns, kind: jax.ShapeDtypeStruct((rows, columns), kind)
    model_rows = rows_of((length, model))
    sums = lambda columns: jax.ShapeDtypeStruct((1, columns), jnp.float32)
    return pl.pallas_call(
        attend_back_kernel,
        grid_spec=pltpu.PrefetchScalarGridSpec(
            num_scalar_prefetch=0,
            grid=(items,),
            in_specs=[
                model_rows,
                model_rows,
                model_rows,
                model_rows,
                whole((1, model)),
                whole(merge.shape),
                rows_of((length, width)),
                whole(head_gain.shape),
                pl.BlockSpec((1, heads, length, length), lambda item, *_: (item, 0, 0, 0)),
                rows_of((length, 3 * width)),
                whole(heads_weight.shape),
            ],
            out_specs=[
                model_rows,
                model_rows,
                rows_of((length, 3 * width)),
                model_rows,
                whole((1, model)),
                whole((1, model)),
                whole((1, model)),
                whole((1, width)),
                whole((1, 3 * width)),
                whole((heads, 2 * length)),
            ],
            scratch_shapes=[pltpu.VMEM((heads, length, length), jnp.float32)],
        ),
        out_shape=[
            out(model, jnp.float32),
            out(model, jnp.bfloat16),
            out(3 * width, jnp.bfloat16),
            out(model, jnp.float32),
            sums(model),
            sums(model),
            sums(model),
            sums(width),
            sums(3 * width),
            jax.ShapeDtypeStruct((heads, 2 * length), jnp.float32),
        ],
        cost_estimate=cost(24),
        name="attend_back",
    )(
        middle,
        own,
        other,
        grad_reduced,
        gain,
        merge,
        mixed,
        head_gain,
        probs,
        heads_low,
        heads_weight,
    )


def stem_back_kernel(
    patches_ref,
    hidden_ref,
    own_ref,
    other_ref,
    grad_middle_ref,
    gain_ref,
    image_ref,
    features_ref,
    mean_ref,
    inverse_ref,
    input_grad_ref,
    grad_embedded_ref,
    grad_stem_ref,
    gain_sum_ref,
    shift_sum_ref,
    stem_gain_ref,
    stem_shift_ref,
):
    item = pl.program_id(0)
    length = hidden_ref.shape[0]
    start_sums(gain_sum_ref, shift_sum_ref, stem_gain_ref, stem_shift_ref)
    normal, inverse = normed(hidden_ref[...])
    grad_first = own_ref[...] + other_ref[...]
    gain_sum_ref[...] += row_sum(grad_first * normal)
    shift_sum_ref[...] += row_sum(grad_first)
    input_grad = grad_middle_ref[...] + norm_back(normal, inverse, grad_first, gain_ref[...])
    input_grad_ref[...] = input_grad
    mask = before(length, patches_ref[item])
    grad_embedded = (input_grad * mask).astype(jnp.bfloat16)
    grad_embedded_ref[...] = grad_embedded
    grad_stem = mult(grad_embedded, image_ref[...], RIGHT)
    grad_stem_ref[...] = grad_stem
    stem_hat = (features_ref[...].astype(jnp.float32) - mean_ref[...]) * inverse_ref[...]
    stem_shift_ref[...] += row_sum(grad_stem)
    stem_gain_ref[...] += row_sum(grad_stem * stem_hat)


def stem_back(
    patches, hidden, own, other, grad_middle, gain, image, features, mean, inverse
):
    items = patches.shape[0]
    rows, model = hidden.shape
    length = rows // items
    channels = features.shape[1]
    out = lambda columns, kind: jax.ShapeDtypeStruct((rows, columns), kind)
    model_rows = rows_of((length, model))
    channel_rows = rows_of((length, channels))
    sums = lambda columns: jax.ShapeDtypeStruct((1, columns), jnp.float32)
    return pl.pallas_call(
        stem_back_kernel,
        grid_spec=pltpu.PrefetchScalarGridSpec(
            num_scalar_prefetch=1,
            grid=(items,),
            in_specs=[
                model_rows,
                model_rows,
                model_rows,
                model_rows,
                whole((1, model)),
                whole(image.shape),
                channel_rows,
                whole((1, channels)),
                whole((1, channels)),
            ],
            out_specs=[
                model_rows,
                model_rows,
                channel_rows,
                whole((1, model)),
                whole((1, model)),
                whole((1, channels)),
                whole((1, channels)),
            ],
        ),
        out_shape=[
            out(model, jnp.float32),
            out(model, jnp.bfloat16),
            out(channels, jnp.float32),
            sums(model),
            sums(model),
            sums(channels),
            sums(channels),
        ],
        cost_estimate=cost(10),
        name="stem_back",
    )(patches, hidden, own, other, grad_middle, gain, image, features, mean, inverse)


def swap_core(values):
    count = lax.axis_size("tensor")
    return lax.ppermute(values, "tensor", [(core, core ^ 1) for core in range(count)])


def exchange(values, bit):
    count = lax.axis_size("dp")
    return lax.ppermute(values, "dp", [(rank, rank ^ (1 << bit)) for rank in range(count)])


def sum_by_doubling(values):
    for bit in range(lax.axis_size("dp").bit_length() - 1):
        values = values + exchange(values, bit)
    return values


class Chain:
    def __init__(self):
        self.token = ()

    def enter(self, *arrays):
        held = lax.optimization_barrier((*self.token, *arrays))
        return held[len(self.token) :]

    def leave(self, *arrays):
        self.token = arrays
        return arrays


def cut(values, side):
    half = values.shape[1] // 2
    return lax.dynamic_slice_in_dim(values, side * half, half, 1)


def spread(side, mine, other):
    return jnp.where(
        side == 1,
        jnp.concatenate([other, mine], axis=1),
        jnp.concatenate([mine, other], axis=1),
    )


def regroup(arrays, count):
    if len(arrays) == count:
        return list(arrays)
    if count == 1:
        return [jnp.concatenate(arrays, axis=0)]
    return list(jnp.split(arrays[0], count, axis=0))


class Stream:
    def __init__(self, chain, paired):
        bits = lax.axis_size("dp").bit_length() - 1
        self.chain = chain
        self.rank = lax.axis_index("dp")
        far = tuple((bit,) for bit in range(2, bits))
        if paired:
            far = tuple((bit, min(bit ^ 1, bits - 1)) for bit in range(2, bits))
        self.plan = ((0, 1), (1, 0)) + far
        self.stage = 0

    def bits(self, stage):
        steps = self.plan + self.plan[::-1]
        return steps[stage]

    def sides(self, stage):
        return [(self.rank >> bit) & 1 for bit in self.bits(stage)]

    def send(self, arrays):
        arrays = self.chain.leave(*arrays)
        self.flight = [exchange(array, bit) for array, bit in zip(arrays, self.bits(self.stage))]

    def launch(self, *parts):
        sides = self.sides(0)
        self.send([part(1 - side) for part, side in zip(parts, sides)])
        self.kept = [part(side) for part, side in zip(parts, sides)]

    def step(self):
        steps = len(self.plan)
        if self.stage == 2 * steps:
            return
        held = self.chain.enter(*self.flight)
        self.stage += 1
        if self.stage < steps:
            count = len(self.bits(self.stage))
            kept, held = regroup(self.kept, count), regroup(held, count)
            sides = self.sides(self.stage)
            pairs = list(zip(kept, held, sides))
            self.send([cut(mine, 1 - side) + cut(other, 1 - side) for mine, other, side in pairs])
            self.kept = [cut(mine, side) + cut(other, side) for mine, other, side in pairs]
        elif self.stage == steps:
            self.values = [mine + other for mine, other in zip(self.kept, held)]
            self.send(self.values)
        else:
            sides = self.sides(self.stage - 1)
            self.last = list(zip(sides, self.values, held))
            if self.stage < 2 * steps:
                values = [spread(*entry) for entry in self.last]
                self.values = regroup(values, len(self.bits(self.stage)))
                self.send(self.values)
            else:
                self.chain.leave(*held)

    def finish(self):
        while self.stage < 2 * len(self.plan):
            self.step()
        return self.last


def piece(entry, start, stop):
    side, mine, other = entry
    whole_rows = spread(side, mine[start:stop], other[start:stop])
    return whole_rows.reshape(-1, whole_rows.shape[2])


def local(
    layer_input,
    patch_features,
    bucket_ids,
    text_lengths,
    upstream,
    query_weight,
    key_weight,
    value_weight,
    merge_weight,
    query_bias,
    value_bias,
    merge_bias,
    head_gain,
    distance_table,
    first_gain,
    first_shift,
    second_gain,
    second_shift,
    expand_weight,
    expand_bias,
    reduce_weight,
    reduce_bias,
    image_weight,
    stem_gain,
    stem_shift,
):
    items = bucket_ids.shape[0]
    rows = layer_input.shape[0]
    length = rows // items
    heads = head_gain.shape[0]
    width = query_weight.shape[1]
    row = lambda vector: vector.reshape(1, -1)
    patches = PATCH_SMALL + (PATCH_LARGE - PATCH_SMALL) * bucket_ids
    valid = patches + text_lengths
    slots = jnp.arange(length, dtype=jnp.int32)
    patch_mask = (slots[None, :] < patches[:, None]).astype(jnp.float32).reshape(rows)
    features = patch_features.astype(jnp.float32)
    masked = features * patch_mask[:, None]
    feature_sum, square_sum, count = sum_by_doubling(
        jnp.stack(
            [
                jnp.sum(masked, axis=0),
                jnp.sum(masked * features, axis=0),
                jnp.full((features.shape[1],), jnp.sum(patch_mask)),
            ]
        )
    )
    bias = distance_bias(distance_table, length)
    heads_weight = jnp.concatenate([query_weight, key_weight, value_weight], axis=1)
    heads_bias = row(jnp.concatenate([query_bias, jnp.zeros_like(query_bias), value_bias]))
    head_gains = row(jnp.repeat(head_gain, HEAD_DIM))
    stem_mean = feature_sum / count
    stem_inverse = lax.rsqrt(square_sum / count - stem_mean * stem_mean + EPSILON)
    stem_hat = (features - stem_mean) * stem_inverse
    stem_low = (stem_hat * stem_gain + stem_shift).astype(jnp.bfloat16)
    embedded = mult(stem_low, image_weight)
    hidden, first_low, heads_low, probs, mixed, scaled_low, branch = attend(
        patches,
        valid,
        layer_input,
        embedded,
        swap_core(embedded),
        row(first_gain),
        row(first_shift),
        heads_weight,
        heads_bias,
        bias,
        head_gains,
        merge_weight,
    )
    (
        middle,
        second_low,
        active_low,
        grad_expanded_low,
        reduced,
        grad_second,
        grad_reduced_low,
        grad_expand_bias,
        grad_reduce_bias,
    ) = feed(
        valid,
        hidden,
        branch,
        swap_core(branch),
        row(merge_bias),
        row(second_gain),
        row(second_shift),
        expand_weight,
        row(expand_bias),
        reduce_weight,
        upstream,
    )
    chain = Chain()
    reduces, expands, others = (Stream(chain, paired) for paired in PAIRED)
    streams = {"R": reduces, "E": expands, "H": others}
    slot = 256
    state = {}

    def reduce_part(at, size):
        def part(side):
            units = lax.dynamic_slice_in_dim(active_low, at + side * (size // 2), size // 2, 1)
            return mult(units, grad_reduced_low, LEFT)[None]

        return part

    def expand_part(at, size):
        def part(side):
            half = second_low.shape[1] // 2
            columns = lax.dynamic_slice_in_dim(state["second"], side * half, half, 1)
            return mult(columns, grad_expanded_low[:, at : at + size], LEFT)[None]

        return part

    def launch_reduces():
        size = active_low.shape[1] // 2
        reduces.launch(reduce_part(0, size), reduce_part(size, size))

    def launch_expands():
        (state["second"],) = chain.enter(second_low)
        size = grad_expanded_low.shape[1] // 2
        expands.launch(expand_part(0, size), expand_part(size, size))

    def run_attend_back():
        (other,) = chain.enter(other_second)
        state["attend"] = attend_back(
            items,
            middle,
            grad_second,
            other,
            grad_reduced_low,
            row(second_gain),
            merge_weight,
            mixed,
            head_gains,
            probs,
            heads_low,
            heads_weight,
        )
        grad_first = state["attend"][3]
        chain.leave(grad_first)
        state["other_first"] = swap_core(grad_first)

    def run_heads():
        first, scaled = chain.enter(first_low, scaled_low)
        grad_branch, grad_heads = state["attend"][1:3]
        split = lambda array, at, size: array[:, at : at + size]
        half = grad_branch.shape[1] // 2
        state["grads"] = chain.leave(
            *(mult(first, split(grad_heads, k * width, width), LEFT) for k in range(3)),
            *(mult(scaled, split(grad_branch, k * half, half), LEFT) for k in range(2)),
        )

    def run_stem_back():
        (other,) = chain.enter(state["other_first"])
        grad_middle, grad_first = state["attend"][0], state["attend"][3]
        state["stem"] = stem_back(
            patches,
            hidden,
            grad_first,
            other,
            grad_middle,
            row(first_gain),
            image_weight,
            patch_features,
            row(stem_mean),
            row(stem_inverse),
        )
        chain.leave(state["stem"][0])

    def run_image():
        (stem,) = chain.enter(stem_low)
        grad_embedded = state["stem"][1]
        half = grad_embedded.shape[1] // 2
        state["image"] = chain.leave(
            *(mult(stem, grad_embedded[:, k * half : k * half + half], LEFT) for k in range(2))
        )

    def launch_others():
        stack = lambda *arrays: [array.reshape(-1, slot, array.shape[1]) for array in arrays]
        grads, image = state["grads"], state["image"]
        left = stack(grads[0], grads[1], image[0])
        merge = jnp.concatenate([grads[3], grads[4]], axis=0)
        right = stack(grads[2], merge, image[1])
        part = lambda pieces: lambda side: jnp.concatenate([cut(p, side) for p in pieces])
        others.launch(part(left), part(right))

    def small_step():
        steps = lax.axis_size("dp").bit_length() - 1
        bit = state.setdefault("bit", 0)
        if bit == 0:
            attend_sums, stem_sums = state["attend"][4:], state["stem"][3:]
            table = [attend_sums[5][head : head + 1] for head in range(heads)]
            state["small"] = (*attend_sums[:5], *stem_sums, grad_expand_bias, grad_reduce_bias)
            state["small"] += tuple(table)
            (packed,) = chain.enter(jnp.concatenate(state["small"], axis=1))
        else:
            packed, moved = chain.enter(state["packed"], state["moved"])
            packed = packed + moved
        (state["packed"],) = chain.leave(packed)
        if bit < steps:
            state["moved"] = exchange(packed, bit)
        state["bit"] = bit + 1

    def swap_reduced():
        (value,) = chain.enter(reduced)
        state["reduced"] = value
        state["other_reduced"] = swap_core(value)

    def run_output():
        (other,) = chain.enter(state["other_reduced"])
        block_output = (middle + (state["reduced"] + other) + reduce_bias).astype(jnp.bfloat16)
        (state["output"],) = chain.leave(block_output)

    def run_patch():
        while state["bit"] <= lax.axis_size("dp").bit_length() - 1:
            small_step()
        at, parts = 0, []
        for entry in state["small"]:
            parts.append(state["packed"][:, at : at + entry.shape[1]])
            at += entry.shape[1]
        state["small"] = parts
        stem_gain_sum, stem_shift_sum = state["small"][7:9]
        (feature,) = chain.enter(patch_features)
        hat = (feature.astype(jnp.float32) - stem_mean) * stem_inverse
        patch_grad = (
            patch_mask[:, None]
            * stem_inverse
            * stem_gain
            * (state["stem"][2] - stem_shift_sum / count - hat * stem_gain_sum / count)
        )
        (state["patch"],) = chain.leave(patch_grad)

    other_second = swap_core(grad_second)
    blocks = {
        "a": run_attend_back,
        "h": run_heads,
        "b": run_stem_back,
        "i": run_image,
        "s": small_step,
        "w": swap_reduced,
        "o": run_output,
        "p": run_patch,
    }
    starts = {"R": launch_reduces, "E": launch_expands, "H": launch_others}
    for step in SCHEDULE.split():
        if step in starts:
            starts.pop(step)()
        elif step in streams:
            streams[step].step()
        else:
            blocks[step]()
    last = {name: stream.finish() for name, stream in streams.items()}
    grad_reduce_weight = jnp.concatenate([piece(entry, 0, 1) for entry in last["R"]], axis=0)
    grad_expand_weight = jnp.concatenate([piece(entry, 0, 1) for entry in last["E"]], axis=1)
    left, right = last["H"]
    model = layer_input.shape[1]
    chunk, deep, image_deep = model // slot, merge_weight.shape[0], image_weight.shape[0] // slot
    grad_query_weight = piece(left, 0, chunk)
    grad_key_weight = piece(left, chunk, 2 * chunk)
    grad_value_weight = piece(right, 0, chunk)
    merge = piece(right, chunk, 2 * chunk)
    grad_merge_weight = jnp.concatenate([merge[:deep], merge[deep:]], axis=1)
    grad_image_weight = jnp.concatenate(
        [
            piece(left, 2 * chunk, 2 * chunk + image_deep),
            piece(right, 2 * chunk, 2 * chunk + image_deep),
        ],
        axis=1,
    )
    (
        grad_second_gain,
        grad_second_shift,
        grad_merge_bias,
        head_sums,
        heads_sums,
        grad_first_gain,
        grad_first_shift,
        grad_stem_gain,
        grad_stem_shift,
        grad_expand_bias,
        grad_reduce_bias,
        *table,
    ) = state["small"]
    grad_head_gain = jnp.sum(head_sums.reshape(heads, HEAD_DIM), axis=1)
    grad_distance_table = jnp.concatenate(table, axis=0)[:, : distance_table.shape[1]]
    block_output, input_grad, patch_grad = state["output"], state["stem"][0], state["patch"]
    return (
        block_output,
        input_grad,
        patch_grad,
        grad_query_weight,
        grad_key_weight,
        grad_value_weight,
        grad_merge_weight,
        heads_sums[0, :width],
        heads_sums[0, 2 * width :],
        grad_merge_bias[0],
        grad_head_gain,
        grad_distance_table,
        grad_first_gain[0],
        grad_first_shift[0],
        grad_second_gain[0],
        grad_second_shift[0],
        grad_expand_weight,
        grad_expand_bias[0],
        grad_reduce_weight,
        grad_reduce_bias[0],
        grad_image_weight,
        grad_stem_gain[0],
        grad_stem_shift[0],
    )


def solution(mesh):
    in_specs = (
        P("dp", None),
        P("dp", "tensor"),
        P("dp"),
        P("dp"),
        P("dp", None),
        P(None, "tensor"),
        P(None, "tensor"),
        P(None, "tensor"),
        P("tensor", None),
        P("tensor"),
        P("tensor"),
        P(),
        P("tensor"),
        P("tensor", None),
        P(),
        P(),
        P(),
        P(),
        P(None, "tensor"),
        P("tensor"),
        P("tensor", None),
        P(),
        P("tensor", None),
        P("tensor"),
        P("tensor"),
    )
    out_specs = (
        P("dp", None),
        P("dp", None),
        P("dp", "tensor"),
        P(None, "tensor"),
        P(None, "tensor"),
        P(None, "tensor"),
        P("tensor", None),
        P("tensor"),
        P("tensor"),
        P(),
        P("tensor"),
        P("tensor", None),
        P(),
        P(),
        P(),
        P(),
        P(None, "tensor"),
        P("tensor"),
        P("tensor", None),
        P(),
        P("tensor", None),
        P("tensor"),
        P("tensor"),
    )
    return jax.shard_map(local, mesh=mesh, in_specs=in_specs, out_specs=out_specs, check_vma=False)
```
